512 devices in a mesh: vocab: 32 (over x, y), hidden: 16 (over z, core).
Axes of the slice: x: 4, y: 8, z: 8, core: 2. Of those that a mesh axis runs over, the one named last changes fastest.
Arguments:
- token_ids: int32 [16384], P('vocab'), may hold values from 0 to 30719
- table: bfloat16 [30720, 128], P('vocab'), may hold values from -0.125 to 0.125
- projection: bfloat16 [128, 4096], P(None, 'hidden'), may hold values from -0.09375 to 0.09375
- grad_out: bfloat16 [16384, 4096], P('vocab', 'hidden'), may hold values from -6 to 6
Outputs:
- table_grad: float32 [30720, 128], P('vocab', 'hidden')
- projection_grad: float32 [128, 4096], P(None, 'hidden')
The draws below stay inside these ranges and needn't reach their ends.
All inputs are finite; a program needn't handle non-finite values.
Results may differ from the reference program's by a relative error of at most 0.018.
Values may be sent and summed in bfloat16 or wider, within the bound.
No kernel may reach another device: no remote copies, remote signals or barrier semaphores. Data moves between devices by JAX's collectives and lax.ppermute only.
A program may use at most 64 MiB of HBM per device.

```python
import jax
import jax.numpy as jnp

D_E = 128
HID = 4096
VOCAB = 30720
TOKENS = 16384
N_HIDDEN = 16


def with_ends(values, key, low, largest):
    spot = [jax.random.randint(jax.random.fold_in(key, axis), (), 0, length) for axis, length in enumerate(values.shape)]
    widest = values.shape.index(max(values.shape))
    next_to = spot[:widest] + [(spot[widest] + 1) % values.shape[widest]] + spot[widest + 1:]
    return values.at[tuple(spot)].set(low).at[tuple(next_to)].set(largest)


def block_levels(own_key, extent, shards, low, largest):
    gain = 1.0
    for axis_at, shards_of in shards:
        heights = jax.random.uniform(jax.random.fold_in(jax.random.fold_in(own_key, 6), axis_at), (shards_of,), jnp.float32, low / len(shards), largest / len(shards))
        gain = gain * jnp.repeat(jnp.exp(heights), extent[axis_at] // shards_of).reshape((-1,) + (1,) * (len(extent) - 1 - axis_at))
    return gain


def noise(key, extent, scale, most, pieces=(), kind=jnp.bfloat16):
    drawn = scale * jax.random.normal(key, extent, jnp.float32)
    if pieces:
        drawn = drawn * block_levels(key, extent, pieces, -0.22, 0.18)
    return jnp.clip(drawn, -most, most).astype(kind)


def setup_inputs(seed: int = 0) -> dict:
    arg_keys = jax.random.split(jax.random.key(seed), 5)
    token_ids = with_ends(jax.random.randint(arg_keys[0], (TOKENS,), 0, VOCAB), jax.random.fold_in(arg_keys[0], 1), 0, VOCAB - 1).astype(jnp.int32)
    table = noise(arg_keys[1], (VOCAB, D_E), (TOKENS ** -0.5), 0.125, ((0, 32),))
    projection = noise(arg_keys[2], (D_E, HID), HID ** -0.5, 0.09375, ((1, 16),))
    grad_out = noise(arg_keys[3], (TOKENS, HID), 1.0, 6.0, ((0, 32), (1, 16)))
    return dict(token_ids=token_ids, table=table, projection=projection, grad_out=grad_out)


def reference(token_ids, table, projection, grad_out):
    embedded = jnp.take(table, token_ids, axis=0)
    projection_grad = jnp.dot(embedded.T, grad_out, preferred_element_type=jnp.float32)
    width = HID // N_HIDDEN
    total = jnp.zeros((grad_out.shape[0], projection.shape[0]), jnp.float32)
    for index in range(N_HIDDEN):
        part_out = grad_out[:, index * width:(index + 1) * width]
        part_proj = projection[:, index * width:(index + 1) * width]
        partial_value = jnp.dot(part_out, part_proj.T, preferred_element_type=jnp.float32)
        total = total + partial_value.astype(jnp.bfloat16).astype(jnp.float32)
    token_grad = total.astype(jnp.bfloat16)
    table_grad = jax.ops.segment_sum(token_grad.astype(jnp.float32), token_ids, num_segments=VOCAB)
    return table_grad, projection_grad
```

```python
import jax
import jax.numpy as jnp
from jax import lax
from jax.experimental import pallas as pl
from jax.experimental.pallas import tpu as pltpu
from jax.sharding import PartitionSpec as P

F32, BF16, I32 = jnp.float32, jnp.bfloat16, jnp.int32
LANES = 128


def run(body, out, *args, flops, limit):
    size = lambda a: a.size * a.dtype.itemsize
    vmem = pl.BlockSpec(memory_space=pltpu.VMEM)
    return pl.pallas_call(
        body,
        out_shape=out,
        in_specs=[vmem] * len(args),
        out_specs=vmem,
        compiler_params=pltpu.CompilerParams(vmem_limit_bytes=limit * 2**20),
        cost_estimate=pl.CostEstimate(
            flops=flops, bytes_accessed=sum(map(size, args)) + size(out), transcendentals=0
        ),
    )(*args)


def exchange(blocks, axis):
    return lax.all_to_all(blocks, axis, split_axis=0, concat_axis=0, tiled=True)


def contract_last(a, b):
    return lax.dot_general(a, b, (((1,), (1,)), ((), ())), preferred_element_type=F32)


def columns_body(table, out):
    width = out.shape[1]
    first = lax.axis_index("hidden") * width
    row = lax.broadcasted_iota(I32, (width, table.shape[1]), 0)
    lane = lax.broadcasted_iota(I32, (width, table.shape[1]), 1)
    pick = (lane == row + first).astype(F32).astype(BF16)
    mine = contract_last(pick, table[...]).astype(BF16)
    for peer in range(out.shape[0]):
        out[peer] = mine


def lookup_body(owners, table, ids, out):
    width = out.shape[1]
    rows = table.shape[1]
    token = ids[...]
    owner = ((token >> 6) * 4370) >> 16
    row = token - owner * rows
    count = token.shape[1]
    hot = (lax.broadcasted_iota(I32, (rows, count), 0) == row).astype(F32).astype(BF16)
    every = jnp.dot(table[...], hot, preferred_element_type=F32)
    total = jnp.zeros((width, count), F32)
    for v in range(owners):
        total = jnp.where(owner == v, every[v * width : (v + 1) * width], total)
    mine = total.astype(BF16)
    for peer in range(out.shape[0]):
        out[peer] = mine


def token_grad_body(partials, ids, out):
    total = partials[0].astype(F32)
    for peer in range(1, partials.shape[0]):
        total = total + partials[peer].astype(F32)
    count = total.shape[1]
    token = ids[...]
    digits = jnp.concatenate([token >> 7, token & 127], axis=0).astype(F32)
    packed = jnp.concatenate([total.astype(BF16), digits.astype(BF16)], axis=1)
    for peer in range(out.shape[0]):
        out[peer] = packed


def segments_body(arrived, out):
    sources, width, _ = arrived.shape
    rows = out.shape[1]
    count = arrived.shape[2] - LANES
    chunks = count // LANES
    groups = -(-rows // LANES)
    first = lax.axis_index("vocab") * rows

    def step(source, total):
        block = arrived[source]
        grad = block[:, :count].astype(F32)
        digits = block[:, count:].astype(F32).astype(I32)
        row = digits[:chunks] * LANES + digits[chunks:] - first
        high, low = row >> 7, row & 127
        left, right = [], []
        for c in range(chunks):
            at = slice(c * LANES, (c + 1) * LANES)
            high_c = jnp.broadcast_to(high[c : c + 1], (width, LANES))
            low_c = jnp.broadcast_to(low[c : c + 1], (LANES, LANES))
            part = grad[:, at]
            left.append(
                jnp.concatenate([jnp.where(high_c == g, part, 0.0) for g in range(groups)], axis=0).astype(BF16)
            )
            right.append(
                (lax.broadcasted_iota(I32, (LANES, LANES), 0) == low_c).astype(F32).astype(BF16)
            )
        return total + contract_last(jnp.concatenate(left, axis=1), jnp.concatenate(right, axis=1))

    total = lax.fori_loop(0, sources, step, jnp.zeros((groups * width, LANES), F32), unroll=4)
    for g in range(groups):
        wide = min(LANES, rows - g * LANES)
        out[:, g * LANES : g * LANES + wide] = total[g * width : (g + 1) * width, :wide]


def projection_body(embedded, grad_out, out):
    result = jnp.dot(embedded[...], grad_out[...], preferred_element_type=F32)
    across = result.shape[1] // LANES
    for piece in range(out.shape[0]):
        i, j = piece // across, piece % across
        out[piece] = result[i * 8 : i * 8 + 8, j * LANES : (j + 1) * LANES].astype(BF16)


def sum_body(arrived, out):
    total = arrived[0].astype(F32)
    for peer in range(1, arrived.shape[0]):
        total = total + arrived[peer].astype(F32)
    mine = total.astype(BF16)
    for peer in range(out.shape[0]):
        out[peer] = mine


def assemble_body(arrived, out):
    across = out.shape[1] // LANES
    for piece in range(arrived.shape[0]):
        i, j = piece // across, piece % across
        out[i * 8 : i * 8 + 8, j * LANES : (j + 1) * LANES] = arrived[piece].astype(F32)


def on_device(token_ids, table, projection, grad_out):
    owners, peers = lax.axis_size("vocab"), lax.axis_size("hidden")
    rows, depth = table.shape
    width = depth // peers
    count = token_ids.shape[0]
    hidden = projection.shape[1]
    S = jax.ShapeDtypeStruct

    columns = run(columns_body, S((owners, width, rows), BF16), table, flops=2 * depth * rows * width, limit=4)
    columns = exchange(columns, "vocab")

    partial_grad = contract_last(projection, grad_out).astype(BF16).reshape(peers, width, count)
    partial_grad = exchange(partial_grad, "hidden")

    def lookup(table, ids, out):
        lookup_body(owners, table, ids, out)

    looked = run(
        lookup,
        S((peers, width, count), BF16),
        columns.reshape(owners * width, rows),
        token_ids.reshape(1, count),
        flops=2 * owners * width * rows * count,
        limit=8,
    )
    embedded = exchange(looked, "hidden").reshape(depth, count)

    packed = run(
        token_grad_body,
        S((owners, width, count + LANES), BF16),
        partial_grad,
        token_ids.reshape(count // LANES, LANES),
        flops=peers * width * count,
        limit=4,
    )
    packed = exchange(packed, "vocab")

    pieces = run(
        projection_body,
        S((owners, 8, depth * hidden // owners // 8), BF16),
        embedded,
        grad_out,
        flops=2 * depth * count * hidden,
        limit=4,
    )
    pieces = exchange(pieces, "vocab")
    summed = run(sum_body, S(pieces.shape, BF16), pieces, flops=pieces.size, limit=4)
    summed = exchange(summed, "vocab")
    table_grad = run(
        segments_body,
        S((width, rows), F32),
        packed,
        flops=2 * owners * count * width * 8 * LANES,
        limit=8,
    )
    projection_grad = run(assemble_body, S((depth, hidden), F32), summed, flops=summed.size, limit=4)
    return table_grad.T, projection_grad


def solution(mesh):
    placed = (P("vocab"), P("vocab", None), P(None, "hidden"), P("vocab", "hidden"))
    return jax.shard_map(
        on_device,
        mesh=mesh,
        in_specs=placed,
        out_specs=(P("vocab", "hidden"), P(None, "hidden")),
        check_vma=False,
    )
```

```python
import jax
import jax.numpy as jnp
from jax import lax
from jax.experimental import pallas as pl
from jax.experimental.pallas import tpu as pltpu
from jax.sharding import PartitionSpec as P

F32, BF16, I32 = jnp.float32, jnp.bfloat16, jnp.int32
LANES, SUBLANES = 128, 8
NEAR = 8


def run(body, out, *args, flops, limit):
    size = lambda a: a.size * a.dtype.itemsize
    vmem = pl.BlockSpec(memory_space=pltpu.VMEM)
    outs = jax.tree.leaves(out)
    return pl.pallas_call(
        body,
        out_shape=out,
        in_specs=[vmem] * len(args),
        out_specs=jax.tree.map(lambda _: vmem, out),
        compiler_params=pltpu.CompilerParams(vmem_limit_bytes=limit * 2**20),
        cost_estimate=pl.CostEstimate(
            flops=flops, bytes_accessed=sum(map(size, [*args, *outs])), transcendentals=0
        ),
    )(*args)


def exchange(blocks, axis, groups=None):
    return lax.all_to_all(blocks, axis, split_axis=0, concat_axis=0, tiled=True, axis_index_groups=groups)


def contract_last(a, b):
    return lax.dot_general(a, b, (((1,), (1,)), ((), ())), preferred_element_type=F32)


def one_hot_rows(which, rows):
    shape = (rows, which.shape[1])
    return (lax.broadcasted_iota(I32, shape, 0) == which).astype(F32).astype(BF16)


def owner_and_row(token, rows):
    owner = ((token >> 6) * 4370) >> 16
    return owner, token - owner * rows


def columns_body(table, out):
    width = out.shape[1]
    first = lax.axis_index("hidden") * width
    shape = (width, table.shape[1])
    lane = lax.broadcasted_iota(I32, shape, 1)
    pick = (lane == lax.broadcasted_iota(I32, shape, 0) + first).astype(F32).astype(BF16)
    mine = contract_last(pick, table[...]).astype(BF16)
    for peer in range(out.shape[0]):
        out[peer] = mine


def lookup_body(owners, table, ids, partials, out):
    width = partials.shape[1]
    count = ids.shape[1]
    owner, row = owner_and_row(ids[...], table.shape[1])
    every = jnp.dot(table[...], one_hot_rows(row, table.shape[1]), preferred_element_type=F32)
    total = jnp.zeros((width, count), F32)
    for v in range(owners):
        total = jnp.where(owner == v, every[v * width : (v + 1) * width], total)
    mine = total.astype(BF16)
    for peer in range(out.shape[0]):
        out[peer, :width] = mine
        out[peer, width:] = partials[peer]


def products_body(rows, arrived, grad_out, ids, out):
    peers = arrived.shape[0]
    width = arrived.shape[1] // 2
    embedded = jnp.concatenate([arrived[p, :width] for p in range(peers)], axis=0)
    product = jnp.dot(embedded, grad_out[...], preferred_element_type=F32).astype(BF16)
    grad = arrived[0, width:].astype(F32)
    for peer in range(1, peers):
        grad = grad + arrived[peer, width:].astype(F32)
    owner, row = owner_and_row(ids[...], rows)
    digits = jnp.concatenate([owner * 8 + (row >> 7), row & 127], axis=0).astype(F32)
    depth = product.shape[0]
    across = product.shape[1] // LANES
    chunks = grad.shape[1] // LANES
    blocks = [product[:, j * LANES : (j + 1) * LANES] for j in range(across)]
    small = [grad[:, c * LANES : (c + 1) * LANES].astype(BF16) for c in range(chunks)] + [digits.astype(BF16)]
    for peer in range(out.shape[0]):
        for j in range(across):
            out[peer, j * depth : (j + 1) * depth] = blocks[j]
        for c in range(chunks + 1):
            at = across * depth + c * SUBLANES
            out[peer, at : at + SUBLANES] = small[c]


def near_sums_body(product_rows, arrived, out):
    near = arrived.shape[0]
    far = out.shape[0]
    chunks = (arrived.shape[1] - product_rows) // SUBLANES - 1
    y = lax.axis_index("vocab") & (NEAR - 1)

    total = arrived[0, :product_rows].astype(F32)
    for peer in range(1, near):
        total = total + arrived[peer, :product_rows].astype(F32)
    total = total.astype(BF16)
    for peer in range(far):
        out[peer, :product_rows] = total

    sums = jnp.zeros((far * 8 * SUBLANES, LANES), F32)
    for peer in range(near):
        at = product_rows + chunks * SUBLANES
        digits = arrived[peer, at : at + SUBLANES].astype(F32).astype(I32)
        high, low = digits[:chunks], digits[chunks:]
        mine = ((high >> 3) & (NEAR - 1)) == y
        group = jnp.where(mine, (high >> 6) * 8 + (high & 7), -1)
        left, right = [], []
        for c in range(chunks):
            start = product_rows + c * SUBLANES
            part = arrived[peer, start : start + SUBLANES].astype(F32)
            group_c = jnp.broadcast_to(group[c : c + 1], part.shape)
            left.append(
                jnp.concatenate([jnp.where(group_c == g, part, 0.0) for g in range(far * 8)], axis=0).astype(BF16)
            )
            right.append(one_hot_rows(low[c : c + 1], LANES))
        sums = sums + contract_last(jnp.concatenate(left, axis=1), jnp.concatenate(right, axis=1))
    sums = sums.astype(BF16)
    for peer in range(far):
        out[peer, product_rows:] = sums[peer * 8 * SUBLANES : (peer + 1) * 8 * SUBLANES]


def far_sums_body(product_rows, arrived, table_grad, projection_grad):
    total = arrived[0].astype(F32)
    for peer in range(1, arrived.shape[0]):
        total = total + arrived[peer].astype(F32)
    depth = projection_grad.shape[0]
    for j in range(projection_grad.shape[1] // LANES):
        projection_grad[:, j * LANES : (j + 1) * LANES] = total[j * depth : (j + 1) * depth]
    rows = table_grad.shape[1]
    for g in range(-(-rows // LANES)):
        at = product_rows + g * SUBLANES
        wide = min(LANES, rows - g * LANES)
        table_grad[:, g * LANES : g * LANES + wide] = total[at : at + SUBLANES, :wide]


def on_device(token_ids, table, projection, grad_out):
    owners, peers = lax.axis_size("vocab"), lax.axis_size("hidden")
    near, far = NEAR, owners // NEAR
    same_x = [[x * near + y for y in range(near)] for x in range(far)]
    same_y = [[x * near + y for x in range(far)] for y in range(near)]
    rows, depth = table.shape
    width = depth // peers
    count = token_ids.shape[0]
    hidden = projection.shape[1]
    product_rows = depth * hidden // LANES
    chunks = count // LANES
    S = jax.ShapeDtypeStruct

    columns = run(columns_body, S((owners, width, rows), BF16), table, flops=2 * depth * rows * width, limit=4)
    columns = exchange(columns, "vocab").reshape(owners * width, rows)

    partials = contract_last(projection, grad_out).astype(BF16).reshape(peers, width, count)

    def lookup(*refs):
        lookup_body(owners, *refs)

    def products(*refs):
        products_body(rows, *refs)

    def near_sums(*refs):
        near_sums_body(product_rows, *refs)

    def far_sums(*refs):
        far_sums_body(product_rows, *refs)

    looked = run(
        lookup,
        S((peers, 2 * width, count), BF16),
        columns,
        token_ids.reshape(1, count),
        partials,
        flops=2 * owners * width * rows * count,
        limit=8,
    )
    looked = exchange(looked, "hidden")

    made = run(
        products,
        S((near, product_rows + (chunks + 1) * SUBLANES, LANES), BF16),
        looked,
        grad_out,
        token_ids.reshape(chunks, LANES),
        flops=2 * depth * count * hidden,
        limit=8,
    )
    made = exchange(made, "vocab", same_x)

    summed = run(
        near_sums,
        S((far, product_rows + 8 * SUBLANES, LANES), BF16),
        made,
        flops=2 * near * count * far * 8 * SUBLANES * LANES,
        limit=8,
    )
    summed = exchange(summed, "vocab", same_y)

    table_grad, projection_grad = run(
        far_sums, (S((width, rows), F32), S((depth, hidden), F32)), summed, flops=summed.size, limit=8
    )
    return table_grad.T, projection_grad


def solution(mesh):
    placed = (P("vocab"), P("vocab", None), P(None, "hidden"), P("vocab", "hidden"))
    return jax.shard_map(
        on_device,
        mesh=mesh,
        in_specs=placed,
        out_specs=(P("vocab", "hidden"), P(None, "hidden")),
        check_vma=False,
    )
```

```python
import jax
import jax.numpy as jnp
from jax import lax
from jax.experimental import pallas as pl
from jax.experimental.pallas import tpu as pltpu
from jax.sharding import PartitionSpec as P

F32, BF16, I32 = jnp.float32, jnp.bfloat16, jnp.int32
LANES, SUBLANES = 128, 8
NEAR = 8


def run(body, out, *args, flops, limit):
    size = lambda a: a.size * a.dtype.itemsize
    vmem = pl.BlockSpec(memory_space=pltpu.VMEM)
    outs = jax.tree.leaves(out)
    return pl.pallas_call(
        body,
        out_shape=out,
        in_specs=[vmem] * len(args),
        out_specs=jax.tree.map(lambda _: vmem, out),
        compiler_params=pltpu.CompilerParams(vmem_limit_bytes=limit * 2**20),
        cost_estimate=pl.CostEstimate(
            flops=flops, bytes_accessed=sum(map(size, [*args, *outs])), transcendentals=0
        ),
    )(*args)


def exchange(blocks, axis, groups=None):
    return lax.all_to_all(blocks, axis, split_axis=0, concat_axis=0, tiled=True, axis_index_groups=groups)


def contract_last(a, b):
    return lax.dot_general(a, b, (((1,), (1,)), ((), ())), preferred_element_type=F32)


def one_hot_rows(which, rows):
    shape = (rows, which.shape[1])
    return (lax.broadcasted_iota(I32, shape, 0) == which).astype(F32).astype(BF16)


def owner_and_row(token, rows):
    owner = ((token >> 6) * 4370) >> 16
    return owner, token - owner * rows


def columns_body(table, out):
    width = out.shape[1]
    first = lax.axis_index("hidden") * width
    shape = (width, table.shape[1])
    lane = lax.broadcasted_iota(I32, shape, 1)
    pick = (lane == lax.broadcasted_iota(I32, shape, 0) + first).astype(F32).astype(BF16)
    mine = contract_last(pick, table[...]).astype(BF16)
    for peer in range(out.shape[0]):
        out[peer] = mine


def lookup_body(owners, table, ids, projection, grad_out, out):
    width = out.shape[1] // 2
    count = ids.shape[1]
    partial = contract_last(projection[...], grad_out[...])
    owner, row = owner_and_row(ids[...], table.shape[1])
    every = jnp.dot(table[...], one_hot_rows(row, table.shape[1]), preferred_element_type=F32)
    total = jnp.zeros((width, count), F32)
    for v in range(owners):
        total = jnp.where(owner == v, every[v * width : (v + 1) * width], total)
    mine = total.astype(BF16)
    for peer in range(out.shape[0]):
        out[peer, :width] = mine
        out[peer, width:] = partial[peer * width : (peer + 1) * width].astype(BF16)


def products_body(rows, arrived, grad_out, ids, out):
    peers = arrived.shape[0]
    width = arrived.shape[1] // 2
    embedded = jnp.concatenate([arrived[p, :width] for p in range(peers)], axis=0)
    product = jnp.dot(embedded, grad_out[...], preferred_element_type=F32).astype(BF16)
    grad = arrived[0, width:].astype(F32)
    for peer in range(1, peers):
        grad = grad + arrived[peer, width:].astype(F32)
    owner, row = owner_and_row(ids[...], rows)
    digits = jnp.concatenate([owner * 8 + (row >> 7), row & 127], axis=0).astype(F32)
    depth = product.shape[0]
    across = product.shape[1] // LANES
    chunks = grad.shape[1] // LANES
    blocks = [product[:, j * LANES : (j + 1) * LANES] for j in range(across)]
    small = [grad[:, c * LANES : (c + 1) * LANES].astype(BF16) for c in range(chunks)] + [digits.astype(BF16)]
    for peer in range(out.shape[0]):
        for j in range(across):
            out[peer, j * depth : (j + 1) * depth] = blocks[j]
        for c in range(chunks + 1):
            at = across * depth + c * SUBLANES
            out[peer, at : at + SUBLANES] = small[c]


def near_sums_body(product_rows, arrived, out):
    near = arrived.shape[0]
    far = out.shape[0]
    chunks = (arrived.shape[1] - product_rows) // SUBLANES - 1
    y = lax.axis_index("vocab") & (NEAR - 1)

    total = arrived[0, :product_rows].astype(F32)
    for peer in range(1, near):
        total = total + arrived[peer, :product_rows].astype(F32)
    total = total.astype(BF16)
    for peer in range(far):
        out[peer, :product_rows] = total

    sums = jnp.zeros((far * 8 * SUBLANES, LANES), F32)
    for peer in range(near):
        at = product_rows + chunks * SUBLANES
        digits = arrived[peer, at : at + SUBLANES].astype(F32).astype(I32)
        high, low = digits[:chunks], digits[chunks:]
        mine = ((high >> 3) & (NEAR - 1)) == y
        group = jnp.where(mine, (high >> 6) * 8 + (high & 7), -1)
        left, right = [], []
        for c in range(chunks):
            start = product_rows + c * SUBLANES
            part = arrived[peer, start : start + SUBLANES].astype(F32)
            group_c = jnp.broadcast_to(group[c : c + 1], part.shape)
            left.append(
                jnp.concatenate([jnp.where(group_c == g, part, 0.0) for g in range(far * 8)], axis=0).astype(BF16)
            )
            right.append(one_hot_rows(low[c : c + 1], LANES))
        sums = sums + contract_last(jnp.concatenate(left, axis=1), jnp.concatenate(right, axis=1))
    sums = sums.astype(BF16)
    for peer in range(far):
        out[peer, product_rows:] = sums[peer * 8 * SUBLANES : (peer + 1) * 8 * SUBLANES]


def far_sums_body(product_rows, arrived, table_grad, projection_grad):
    total = arrived[0].astype(F32)
    for peer in range(1, arrived.shape[0]):
        total = total + arrived[peer].astype(F32)
    depth = projection_grad.shape[0]
    for j in range(projection_grad.shape[1] // LANES):
        projection_grad[:, j * LANES : (j + 1) * LANES] = total[j * depth : (j + 1) * depth]
    rows = table_grad.shape[1]
    for g in range(-(-rows // LANES)):
        at = product_rows + g * SUBLANES
        wide = min(LANES, rows - g * LANES)
        table_grad[:, g * LANES : g * LANES + wide] = total[at : at + SUBLANES, :wide]


def on_device(token_ids, table, projection, grad_out):
    owners, peers = lax.axis_size("vocab"), lax.axis_size("hidden")
    near, far = NEAR, owners // NEAR
    same_x = [[x * near + y for y in range(near)] for x in range(far)]
    same_y = [[x * near + y for x in range(far)] for y in range(near)]
    rows, depth = table.shape
    width = depth // peers
    count = token_ids.shape[0]
    hidden = projection.shape[1]
    product_rows = depth * hidden // LANES
    chunks = count // LANES
    S = jax.ShapeDtypeStruct

    columns = run(columns_body, S((owners, width, rows), BF16), table, flops=2 * depth * rows * width, limit=4)
    columns = exchange(columns, "vocab").reshape(owners * width, rows)

    def lookup(*refs):
        lookup_body(owners, *refs)

    def products(*refs):
        products_body(rows, *refs)

    def near_sums(*refs):
        near_sums_body(product_rows, *refs)

    def far_sums(*refs):
        far_sums_body(product_rows, *refs)

    looked = run(
        lookup,
        S((peers, 2 * width, count), BF16),
        columns,
        token_ids.reshape(1, count),
        projection,
        grad_out,
        flops=2 * owners * width * rows * count + 2 * depth * count * hidden,
        limit=8,
    )
    looked = exchange(looked, "hidden")

    made = run(
        products,
        S((near, product_rows + (chunks + 1) * SUBLANES, LANES), BF16),
        looked,
        grad_out,
        token_ids.reshape(chunks, LANES),
        flops=2 * depth * count * hidden,
        limit=8,
    )
    made = exchange(made, "vocab", same_x)

    summed = run(
        near_sums,
        S((far, product_rows + 8 * SUBLANES, LANES), BF16),
        made,
        flops=2 * near * count * far * 8 * SUBLANES * LANES,
        limit=8,
    )
    summed = exchange(summed, "vocab", same_y)

    table_grad, projection_grad = run(
        far_sums, (S((width, rows), F32), S((depth, hidden), F32)), summed, flops=summed.size, limit=8
    )
    return table_grad.T, projection_grad


def solution(mesh):
    placed = (P("vocab"), P("vocab", None), P(None, "hidden"), P("vocab", "hidden"))
    return jax.shard_map(
        on_device,
        mesh=mesh,
        in_specs=placed,
        out_specs=(P("vocab", "hidden"), P(None, "hidden")),
        check_vma=False,
    )
```

```python
import jax
import jax.numpy as jnp
from jax import lax
from jax.experimental import pallas as pl
from jax.experimental.pallas import tpu as pltpu
from jax.sharding import PartitionSpec as P

F32, BF16, I32 = jnp.float32, jnp.bfloat16, jnp.int32
LANES, SUBLANES = 128, 8
ALONG_Y = 8


def run(body, out, *args, flops, limit, space=pltpu.VMEM, scratch=()):
    size = lambda a: a.size * a.dtype.itemsize
    vmem = pl.BlockSpec(memory_space=pltpu.VMEM)
    outs = jax.tree.leaves(out)
    if space != pltpu.VMEM:
        args = [pltpu.with_memory_space_constraint(a, space) for a in args]
    return pl.pallas_call(
        body,
        out_shape=out,
        in_specs=[pl.BlockSpec(memory_space=space)] * len(args),
        out_specs=jax.tree.map(lambda _: vmem, out),
        scratch_shapes=scratch,
        compiler_params=pltpu.CompilerParams(vmem_limit_bytes=limit * 2**20),
        cost_estimate=pl.CostEstimate(
            flops=flops, bytes_accessed=sum(map(size, [*args, *outs])), transcendentals=0
        ),
    )(*args)


def exchange(blocks, axis, groups=None):
    return lax.all_to_all(blocks, axis, split_axis=0, concat_axis=0, tiled=True, axis_index_groups=groups)


def contract_last(a, b):
    return lax.dot_general(a, b, (((1,), (1,)), ((), ())), preferred_element_type=F32)


def one_hot_rows(which, rows):
    shape = (rows, which.shape[1])
    return (lax.broadcasted_iota(I32, shape, 0) == which).astype(F32).astype(BF16)


def owner_and_row(token, rows):
    owner = ((token >> 6) * 4370) >> 16
    return owner, token - owner * rows


def columns_body(table_there, ids_there, out, places, digits, table, ids, arrivals):
    copies = [
        pltpu.make_async_copy(table_there, table, arrivals.at[0]),
        pltpu.make_async_copy(ids_there, ids, arrivals.at[1]),
    ]
    for copy in copies:
        copy.start()
    copies[1].wait()
    owner, row = owner_and_row(ids[...], table.shape[0])
    digits[...] = jnp.concatenate([owner * 8 + (row >> 7), row & 127], axis=0).astype(F32)
    for c in range(ids.shape[0]):
        at = slice(c * LANES, (c + 1) * LANES)
        places[0:1, at] = owner[c : c + 1]
        places[1:2, at] = row[c : c + 1]
    copies[0].wait()
    width = out.shape[1]
    first = lax.axis_index("hidden") * width
    shape = (width, table.shape[1])
    lane = lax.broadcasted_iota(I32, shape, 1)
    pick = (lane == lax.broadcasted_iota(I32, shape, 0) + first).astype(F32).astype(BF16)
    mine = contract_last(pick, table[...]).astype(BF16)
    for peer in range(out.shape[0]):
        out[peer] = mine


def lookup_body(owners, table, places, projection, grad_out, out):
    width = out.shape[1] // 2
    count = places.shape[1]
    partial = contract_last(projection[...], grad_out[...])
    owner, row = places[0:1, :], places[1:2, :]
    every = jnp.dot(table[...], one_hot_rows(row, table.shape[1]), preferred_element_type=F32)
    total = jnp.zeros((width, count), F32)
    for v in range(owners):
        total = jnp.where(owner == v, every[v * width : (v + 1) * width], total)
    mine = total.astype(BF16)
    for peer in range(out.shape[0]):
        out[peer, :width] = mine
        out[peer, width:] = partial[peer * width : (peer + 1) * width].astype(BF16)


def rows_of_lanes(value):
    return [value[:, j : j + LANES] for j in range(0, value.shape[1], LANES)]


def products_body(arrived, grad_out, digits, out):
    peers = arrived.shape[0]
    width = arrived.shape[1] // 2
    embedded = jnp.concatenate([arrived[p, :width] for p in range(peers)], axis=0)
    product = jnp.dot(embedded, grad_out[...], preferred_element_type=F32)
    product = jnp.concatenate(rows_of_lanes(product), axis=0).astype(BF16)
    grad = arrived[0, width:].astype(F32)
    for peer in range(1, peers):
        grad = grad + arrived[peer, width:].astype(F32)
    small = [part.astype(BF16) for part in [*rows_of_lanes(grad), digits[...]]]
    members = out.shape[0]
    piece = product.shape[0] // members
    for peer in range(members):
        out[peer, :piece] = product[peer * piece : (peer + 1) * piece]
        for c, part in enumerate(small):
            at = piece + c * SUBLANES
            out[peer, at : at + SUBLANES] = part


def group_sums_body(piece, arrived, out):
    members, owners = arrived.shape[0], out.shape[0]
    chunks = (arrived.shape[1] - piece) // SUBLANES - 1
    vocab = lax.axis_index("vocab")
    member = (vocab // ALONG_Y) * 2 + (vocab & 1)

    total = arrived[0, :piece].astype(F32)
    for peer in range(1, members):
        total = total + arrived[peer, :piece].astype(F32)
    total = total.astype(BF16)

    sums = jnp.zeros((owners * SUBLANES, LANES), F32)
    for peer in range(members):
        at = piece + chunks * SUBLANES
        digits = arrived[peer, at : at + SUBLANES].astype(F32).astype(I32)
        high, low = digits[:chunks], digits[chunks:]
        owner = jnp.where((high & 7) == member, high >> 3, -1)
        left, right = [], []
        for c in range(chunks):
            start = piece + c * SUBLANES
            part = arrived[peer, start : start + SUBLANES].astype(F32)
            owner_c = jnp.broadcast_to(owner[c : c + 1], part.shape)
            left.append(
                jnp.concatenate([jnp.where(owner_c == v, part, 0.0) for v in range(owners)], axis=0).astype(BF16)
            )
            right.append(one_hot_rows(low[c : c + 1], LANES))
        sums = sums + contract_last(jnp.concatenate(left, axis=1), jnp.concatenate(right, axis=1))
    sums = sums.astype(BF16)
    for v in range(owners):
        out[v, :piece] = total
        out[v, piece:] = sums[v * SUBLANES : (v + 1) * SUBLANES]


def last_sums_body(piece, arrived, table_grad, projection_grad):
    owners = arrived.shape[0]
    depth = projection_grad.shape[0]
    rows = table_grad.shape[1]
    members = depth * projection_grad.shape[1] // LANES // piece
    for member in range(members):
        first = (member >> 1) * ALONG_Y + (member & 1)
        total = arrived[first].astype(F32)
        for peer in range(first + 2, first + ALONG_Y, 2):
            total = total + arrived[peer].astype(F32)
        at, lane = member * piece % depth, member * piece // depth * LANES
        projection_grad[at : at + piece, lane : lane + LANES] = total[:piece]
        wide = min(LANES, rows - member * LANES)
        table_grad[:, member * LANES : member * LANES + wide] = total[piece:, :wide]


def on_device(token_ids, table, projection, grad_out):
    owners, peers = lax.axis_size("vocab"), lax.axis_size("hidden")
    along_x = owners // ALONG_Y
    members = 2 * along_x
    groups = [
        [x * ALONG_Y + y + bit for x in range(along_x) for bit in range(2)] for y in range(0, ALONG_Y, 2)
    ]
    rows, depth = table.shape
    width = depth // peers
    count = token_ids.shape[0]
    hidden = projection.shape[1]
    piece = depth * hidden // LANES // members
    chunks = count // LANES
    S = jax.ShapeDtypeStruct

    by_lane = token_ids.reshape(chunks, LANES)
    columns, places, digits = run(
        columns_body,
        (S((owners, width, rows), BF16), S((2, count), I32), S((2 * chunks, LANES), F32)),
        table,
        by_lane,
        flops=2 * depth * rows * width,
        limit=4,
        space=pltpu.HBM,
        scratch=[
            pltpu.VMEM(table.shape, table.dtype),
            pltpu.VMEM(by_lane.shape, I32),
            pltpu.SemaphoreType.DMA((2,)),
        ],
    )
    columns = exchange(columns, "vocab").reshape(owners * width, rows)

    def lookup(*refs):
        lookup_body(owners, *refs)

    def group_sums(*refs):
        group_sums_body(piece, *refs)

    def last_sums(*refs):
        last_sums_body(piece, *refs)

    looked = run(
        lookup,
        S((peers, 2 * width, count), BF16),
        columns,
        places,
        projection,
        grad_out,
        flops=2 * owners * width * rows * count + 2 * depth * count * hidden,
        limit=8,
    )
    looked = exchange(looked, "hidden")

    made = run(
        products_body,
        S((members, piece + (chunks + 1) * SUBLANES, LANES), BF16),
        looked,
        grad_out,
        digits,
        flops=2 * depth * count * hidden,
        limit=8,
    )
    made = exchange(made, "vocab", groups)

    summed = run(
        group_sums,
        S((owners, piece + SUBLANES, LANES), BF16),
        made,
        flops=2 * members * count * owners * SUBLANES * LANES,
        limit=8,
    )
    summed = exchange(summed, "vocab")

    table_grad, projection_grad = run(
        last_sums, (S((width, rows), F32), S((depth, hidden), F32)), summed, flops=summed.size, limit=8
    )
    return table_grad.T, projection_grad


def solution(mesh):
    placed = (P("vocab"), P("vocab", None), P(None, "hidden"), P("vocab", "hidden"))
    return jax.shard_map(
        on_device,
        mesh=mesh,
        in_specs=placed,
        out_specs=(P("vocab", "hidden"), P(None, "hidden")),
        check_vma=False,
    )
```

```python
import jax
import jax.numpy as jnp
from jax import lax
from jax.experimental import pallas as pl
from jax.experimental.pallas import tpu as pltpu
from jax.sharding import PartitionSpec as P

F32, BF16, I32 = jnp.float32, jnp.bfloat16, jnp.int32
LANES, SUBLANES = 128, 8
CUT = 256
ALONG_Y = 8


def run(body, out, *args, flops, limit, space=pltpu.VMEM, scratch=()):
    size = lambda a: a.size * a.dtype.itemsize
    vmem = pl.BlockSpec(memory_space=pltpu.VMEM)
    outs = jax.tree.leaves(out)
    if space != pltpu.VMEM:
        args = [pltpu.with_memory_space_constraint(a, space) for a in args]
    return pl.pallas_call(
        body,
        out_shape=out,
        in_specs=[pl.BlockSpec(memory_space=space)] * len(args),
        out_specs=jax.tree.map(lambda _: vmem, out),
        scratch_shapes=scratch,
        compiler_params=pltpu.CompilerParams(vmem_limit_bytes=limit * 2**20),
        cost_estimate=pl.CostEstimate(
            flops=flops, bytes_accessed=sum(map(size, [*args, *outs])), transcendentals=0
        ),
    )(*args)


def exchange(blocks, axis, groups=None):
    return lax.all_to_all(blocks, axis, split_axis=0, concat_axis=0, tiled=True, axis_index_groups=groups)


def contract_last(a, b):
    return lax.dot_general(a, b, (((1,), (1,)), ((), ())), preferred_element_type=F32)


def small(value):
    return value.astype(F32).astype(BF16)


def row_numbers(rows, count):
    return small(lax.broadcasted_iota(I32, (rows, count), 0))


def one_hot_rows(which, numbers):
    which = jnp.broadcast_to(small(which), numbers.shape)
    return jnp.where(which == numbers, jnp.ones_like(numbers), jnp.zeros_like(numbers))


def owner_and_row(token, rows):
    owner = ((token >> 6) * 4370) >> 16
    return owner, token - owner * rows


def columns_body(table_there, ids_there, out, places, digits, table, ids, arrivals):
    rows = table.shape[0]
    cuts = [(at, min(CUT, rows - at)) for at in range(0, rows, CUT)]
    copies = [
        pltpu.make_async_copy(table_there.at[pl.ds(at, size)], table.at[pl.ds(at, size)], arrivals.at[i])
        for i, (at, size) in enumerate(cuts)
    ]
    ids_copy = pltpu.make_async_copy(ids_there, ids, arrivals.at[len(cuts)])
    for copy in [*copies, ids_copy]:
        copy.start()
    ids_copy.wait()
    owner, row = owner_and_row(ids[...], table.shape[0])
    digits[...] = jnp.concatenate([owner * 8 + (row >> 7), row & 127], axis=0).astype(F32)
    for c in range(ids.shape[0]):
        at = slice(c * LANES, (c + 1) * LANES)
        places[0:1, at] = owner[c : c + 1]
        places[1:2, at] = row[c : c + 1]
    width = out.shape[1]
    first = lax.axis_index("hidden") * width
    shape = (width, table.shape[1])
    lane = lax.broadcasted_iota(I32, shape, 1)
    pick = (lane == lax.broadcasted_iota(I32, shape, 0) + first).astype(F32).astype(BF16)
    for copy, (at, size) in zip(copies, cuts):
        copy.wait()
        mine = contract_last(pick, table[at : at + size]).astype(BF16)
        for peer in range(out.shape[0]):
            out[peer, :, at : at + size] = mine


def lookup_body(owners, table, places, projection, grad_out, out):
    width = out.shape[1] // 2
    count = places.shape[1]
    partial = contract_last(projection[...], grad_out[...])
    owner, row = places[0:1, :], places[1:2, :]
    numbers = row_numbers(LANES, count)
    rows = table.shape[1]
    hot = [one_hot_rows(row - at, numbers[: min(LANES, rows - at)]) for at in range(0, rows, LANES)]
    every = jnp.dot(table[...], jnp.concatenate(hot, axis=0), preferred_element_type=F32)
    total = jnp.zeros((width, count), F32)
    for v in range(owners):
        total = jnp.where(owner == v, every[v * width : (v + 1) * width], total)
    mine = total.astype(BF16)
    for peer in range(out.shape[0]):
        out[peer, :width] = mine
        out[peer, width:] = partial[peer * width : (peer + 1) * width].astype(BF16)


def rows_of_lanes(value):
    return [value[:, j : j + LANES] for j in range(0, value.shape[1], LANES)]


def products_body(arrived, grad_out, digits, out):
    peers = arrived.shape[0]
    width = arrived.shape[1] // 2
    embedded = jnp.concatenate([arrived[p, :width] for p in range(peers)], axis=0)
    product = jnp.dot(embedded, grad_out[...], preferred_element_type=F32)
    product = jnp.concatenate(rows_of_lanes(product), axis=0).astype(BF16)
    grad = arrived[0, width:].astype(F32)
    for peer in range(1, peers):
        grad = grad + arrived[peer, width:].astype(F32)
    lines = [part.astype(BF16) for part in [*rows_of_lanes(grad), digits[...]]]
    members = out.shape[0]
    piece = product.shape[0] // members
    for peer in range(members):
        out[peer, :piece] = product[peer * piece : (peer + 1) * piece]
        for c, part in enumerate(lines):
            at = piece + c * SUBLANES
            out[peer, at : at + SUBLANES] = part


def group_sums_body(piece, arrived, out):
    members, owners = arrived.shape[0], out.shape[0]
    chunks = (arrived.shape[1] - piece) // SUBLANES - 1
    vocab = lax.axis_index("vocab")
    member = (vocab // ALONG_Y) * 2 + (vocab & 1)

    total = arrived[0, :piece].astype(F32)
    for peer in range(1, members):
        total = total + arrived[peer, :piece].astype(F32)
    total = total.astype(BF16)

    numbers = row_numbers(LANES, LANES)
    second = small(lax.broadcasted_iota(I32, (2 * SUBLANES, LANES), 0) >> 3)
    sums = jnp.zeros((owners * SUBLANES, LANES), F32)
    for peer in range(members):
        at = piece + chunks * SUBLANES
        digits = arrived[peer, at : at + SUBLANES].astype(F32).astype(I32)
        high, low = digits[:chunks], digits[chunks:]
        owner = jnp.where((high & 7) == member, high >> 3, -2)
        left, right = [], []
        for c in range(chunks):
            start = piece + c * SUBLANES
            part = arrived[peer, start : start + SUBLANES]
            twice = jnp.concatenate([part, part], axis=0)
            nought = jnp.zeros_like(twice)
            pair = jnp.broadcast_to(small(owner[c : c + 1]), twice.shape) - second
            left.append(jnp.concatenate([jnp.where(pair == v, twice, nought) for v in range(0, owners, 2)], axis=0))
            right.append(one_hot_rows(low[c : c + 1], numbers))
        sums = sums + contract_last(jnp.concatenate(left, axis=1), jnp.concatenate(right, axis=1))
    sums = sums.astype(BF16)
    for v in range(owners):
        out[v, :piece] = total
        out[v, piece:] = sums[v * SUBLANES : (v + 1) * SUBLANES]


def last_sums_body(piece, arrived, table_grad, projection_grad):
    owners = arrived.shape[0]
    depth = projection_grad.shape[0]
    rows = table_grad.shape[1]
    members = depth * projection_grad.shape[1] // LANES // piece
    for member in range(members):
        first = (member >> 1) * ALONG_Y + (member & 1)
        total = arrived[first].astype(F32)
        for peer in range(first + 2, first + ALONG_Y, 2):
            total = total + arrived[peer].astype(F32)
        at, lane = member * piece % depth, member * piece // depth * LANES
        projection_grad[at : at + piece, lane : lane + LANES] = total[:piece]
        wide = min(LANES, rows - member * LANES)
        table_grad[:, member * LANES : member * LANES + wide] = total[piece:, :wide]


def on_device(token_ids, table, projection, grad_out):
    owners, peers = lax.axis_size("vocab"), lax.axis_size("hidden")
    along_x = owners // ALONG_Y
    members = 2 * along_x
    groups = [
        [x * ALONG_Y + y + bit for x in range(along_x) for bit in range(2)] for y in range(0, ALONG_Y, 2)
    ]
    rows, depth = table.shape
    width = depth // peers
    count = token_ids.shape[0]
    hidden = projection.shape[1]
    piece = depth * hidden // LANES // members
    chunks = count // LANES
    S = jax.ShapeDtypeStruct

    by_lane = token_ids.reshape(chunks, LANES)
    columns, places, digits = run(
        columns_body,
        (S((owners, width, rows), BF16), S((2, count), I32), S((2 * chunks, LANES), F32)),
        table,
        by_lane,
        flops=2 * depth * rows * width,
        limit=4,
        space=pltpu.HBM,
        scratch=[
            pltpu.VMEM(table.shape, table.dtype),
            pltpu.VMEM(by_lane.shape, I32),
            pltpu.SemaphoreType.DMA((-(-rows // CUT) + 1,)),
        ],
    )
    columns = exchange(columns, "vocab").reshape(owners * width, rows)

    def lookup(*refs):
        lookup_body(owners, *refs)

    def group_sums(*refs):
        group_sums_body(piece, *refs)

    def last_sums(*refs):
        last_sums_body(piece, *refs)

    looked = run(
        lookup,
        S((peers, 2 * width, count), BF16),
        columns,
        places,
        projection,
        grad_out,
        flops=2 * owners * width * rows * count + 2 * depth * count * hidden,
        limit=8,
    )
    looked = exchange(looked, "hidden")

    made = run(
        products_body,
        S((members, piece + (chunks + 1) * SUBLANES, LANES), BF16),
        looked,
        grad_out,
        digits,
        flops=2 * depth * count * hidden,
        limit=8,
    )
    made = exchange(made, "vocab", groups)

    summed = run(
        group_sums,
        S((owners, piece + SUBLANES, LANES), BF16),
        made,
        flops=2 * members * count * owners * SUBLANES * LANES,
        limit=8,
    )
    summed = exchange(summed, "vocab")

    table_grad, projection_grad = run(
        last_sums, (S((width, rows), F32), S((depth, hidden), F32)), summed, flops=summed.size, limit=8
    )
    return table_grad.T, projection_grad


def solution(mesh):
    placed = (P("vocab"), P("vocab", None), P(None, "hidden"), P("vocab", "hidden"))
    return jax.shard_map(
        on_device,
        mesh=mesh,
        in_specs=placed,
        out_specs=(P("vocab", "hidden"), P(None, "hidden")),
        check_vma=False,
    )
```

```python
import jax
import jax.numpy as jnp
from jax import lax
from jax.experimental import pallas as pl
from jax.experimental.pallas import tpu as pltpu
from jax.sharding import PartitionSpec as P

F32, BF16, I32 = jnp.float32, jnp.bfloat16, jnp.int32
LANES, SUBLANES = 128, 8
ALONG_Y = 8


def run(body, out, *args, flops, limit, space=pltpu.VMEM, scratch=()):
    size = lambda a: a.size * a.dtype.itemsize
    vmem = pl.BlockSpec(memory_space=pltpu.VMEM)
    outs = jax.tree.leaves(out)
    if space != pltpu.VMEM:
        args = [pltpu.with_memory_space_constraint(a, space) for a in args]
    return pl.pallas_call(
        body,
        out_shape=out,
        in_specs=[pl.BlockSpec(memory_space=space)] * len(args),
        out_specs=jax.tree.map(lambda _: vmem, out),
        scratch_shapes=scratch,
        compiler_params=pltpu.CompilerParams(vmem_limit_bytes=limit * 2**20),
        cost_estimate=pl.CostEstimate(
            flops=flops, bytes_accessed=sum(map(size, [*args, *outs])), transcendentals=0
        ),
    )(*args)


def exchange(blocks, axis, groups=None):
    return lax.all_to_all(blocks, axis, split_axis=0, concat_axis=0, tiled=True, axis_index_groups=groups)


def contract_last(a, b):
    return lax.dot_general(a, b, (((1,), (1,)), ((), ())), preferred_element_type=F32)


def small(value):
    return value.astype(F32).astype(BF16)


def row_numbers(rows, count):
    return small(lax.broadcasted_iota(I32, (rows, count), 0))


def one_hot_rows(which, numbers):
    which = jnp.broadcast_to(small(which), numbers.shape)
    return jnp.where(which == numbers, jnp.ones_like(numbers), jnp.zeros_like(numbers))


def owner_and_row(token, rows):
    owner = ((token >> 6) * 4370) >> 16
    return owner, token - owner * rows


def columns_body(table_there, ids_there, out, places, digits, table, ids, arrivals):
    copies = [
        pltpu.make_async_copy(table_there, table, arrivals.at[0]),
        pltpu.make_async_copy(ids_there, ids, arrivals.at[1]),
    ]
    for copy in copies:
        copy.start()
    copies[1].wait()
    owner, row = owner_and_row(ids[...], table.shape[0])
    digits[...] = jnp.concatenate([owner * 8 + (row >> 7), row & 127], axis=0).astype(F32)
    for c in range(ids.shape[0]):
        at = slice(c * LANES, (c + 1) * LANES)
        places[0:1, at] = owner[c : c + 1]
        places[1:2, at] = row[c : c + 1]
    copies[0].wait()
    width = out.shape[1]
    first = lax.axis_index("hidden") * width
    shape = (width, table.shape[1])
    lane = lax.broadcasted_iota(I32, shape, 1)
    pick = (lane == lax.broadcasted_iota(I32, shape, 0) + first).astype(F32).astype(BF16)
    mine = contract_last(pick, table[...]).astype(BF16)
    for peer in range(out.shape[0]):
        out[peer] = mine


def lookup_body(owners, table, places, projection, grad_out, out):
    width = out.shape[1] // 2
    count = places.shape[1]
    partial = contract_last(projection[...], grad_out[...])
    owner, row = places[0:1, :], places[1:2, :]
    numbers = row_numbers(LANES, count)
    rows = table.shape[1]
    hot = [one_hot_rows(row - at, numbers[: min(LANES, rows - at)]) for at in range(0, rows, LANES)]
    every = jnp.dot(table[...], jnp.concatenate(hot, axis=0), preferred_element_type=F32)
    total = jnp.zeros((width, count), F32)
    for v in range(owners):
        total = jnp.where(owner == v, every[v * width : (v + 1) * width], total)
    mine = total.astype(BF16)
    for peer in range(out.shape[0]):
        out[peer, :width] = mine
        out[peer, width:] = partial[peer * width : (peer + 1) * width].astype(BF16)


def rows_of_lanes(value):
    return [value[:, j : j + LANES] for j in range(0, value.shape[1], LANES)]


def products_body(arrived, grad_out, digits, out):
    peers = arrived.shape[0]
    width = arrived.shape[1] // 2
    embedded = jnp.concatenate([arrived[p, :width] for p in range(peers)], axis=0)
    product = jnp.dot(embedded, grad_out[...], preferred_element_type=F32)
    product = jnp.concatenate(rows_of_lanes(product), axis=0).astype(BF16)
    grad = arrived[0, width:].astype(F32)
    for peer in range(1, peers):
        grad = grad + arrived[peer, width:].astype(F32)
    lines = [part.astype(BF16) for part in [*rows_of_lanes(grad), digits[...]]]
    members = out.shape[0]
    piece = product.shape[0] // members
    for peer in range(members):
        out[peer, :piece] = product[peer * piece : (peer + 1) * piece]
        for c, part in enumerate(lines):
            at = piece + c * SUBLANES
            out[peer, at : at + SUBLANES] = part


def group_sums_body(piece, arrived, out):
    members, owners = arrived.shape[0], out.shape[0]
    chunks = (arrived.shape[1] - piece) // SUBLANES - 1
    vocab = lax.axis_index("vocab")
    member = (vocab // ALONG_Y) * 2 + (vocab & 1)

    total = arrived[0, :piece].astype(F32)
    for peer in range(1, members):
        total = total + arrived[peer, :piece].astype(F32)
    total = total.astype(BF16)

    numbers = row_numbers(2 * LANES, LANES)
    second = small(lax.broadcasted_iota(I32, (2 * SUBLANES, LANES), 0) >> 3)
    sums = jnp.zeros((owners // 2 * SUBLANES, 2 * LANES), F32)
    for peer in range(members):
        at = piece + chunks * SUBLANES
        digits = arrived[peer, at : at + SUBLANES].astype(F32).astype(I32)
        high, low = digits[:chunks], digits[chunks:]
        two_owners = jnp.where((high & 7) == member, high >> 4, -2)
        row = ((high >> 3) & 1) * LANES + low
        left, right = [], []
        for c in range(chunks):
            start = piece + c * SUBLANES
            part = arrived[peer, start : start + SUBLANES]
            twice = jnp.concatenate([part, part], axis=0)
            nought = jnp.zeros_like(twice)
            pair = jnp.broadcast_to(small(two_owners[c : c + 1]), twice.shape) - second
            left.append(
                jnp.concatenate([jnp.where(pair == v, twice, nought) for v in range(0, owners // 2, 2)], axis=0)
            )
            right.append(one_hot_rows(row[c : c + 1], numbers))
        sums = sums + contract_last(jnp.concatenate(left, axis=1), jnp.concatenate(right, axis=1))
    sums = sums.astype(BF16)
    for v in range(owners):
        out[v, :piece] = total
        at, lane = v // 2 * SUBLANES, v % 2 * LANES
        out[v, piece:] = sums[at : at + SUBLANES, lane : lane + LANES]


def last_sums_body(piece, arrived, table_grad, projection_grad):
    owners = arrived.shape[0]
    depth = projection_grad.shape[0]
    rows = table_grad.shape[1]
    members = depth * projection_grad.shape[1] // LANES // piece
    for member in range(members):
        first = (member >> 1) * ALONG_Y + (member & 1)
        total = arrived[first].astype(F32)
        for peer in range(first + 2, first + ALONG_Y, 2):
            total = total + arrived[peer].astype(F32)
        at, lane = member * piece % depth, member * piece // depth * LANES
        projection_grad[at : at + piece, lane : lane + LANES] = total[:piece]
        wide = min(LANES, rows - member * LANES)
        table_grad[:, member * LANES : member * LANES + wide] = total[piece:, :wide]


def on_device(token_ids, table, projection, grad_out):
    owners, peers = lax.axis_size("vocab"), lax.axis_size("hidden")
    along_x = owners // ALONG_Y
    members = 2 * along_x
    groups = [
        [x * ALONG_Y + y + bit for x in range(along_x) for bit in range(2)] for y in range(0, ALONG_Y, 2)
    ]
    rows, depth = table.shape
    width = depth // peers
    count = token_ids.shape[0]
    hidden = projection.shape[1]
    piece = depth * hidden // LANES // members
    chunks = count // LANES
    S = jax.ShapeDtypeStruct

    by_lane = token_ids.reshape(chunks, LANES)
    columns, places, digits = run(
        columns_body,
        (S((owners, width, rows), BF16), S((2, count), I32), S((2 * chunks, LANES), F32)),
        table,
        by_lane,
        flops=2 * depth * rows * width,
        limit=4,
        space=pltpu.HBM,
        scratch=[
            pltpu.VMEM(table.shape, table.dtype),
            pltpu.VMEM(by_lane.shape, I32),
            pltpu.SemaphoreType.DMA((2,)),
        ],
    )
    columns = exchange(columns, "vocab").reshape(owners * width, rows)

    def lookup(*refs):
        lookup_body(owners, *refs)

    def group_sums(*refs):
        group_sums_body(piece, *refs)

    def last_sums(*refs):
        last_sums_body(piece, *refs)

    looked = run(
        lookup,
        S((peers, 2 * width, count), BF16),
        columns,
        places,
        projection,
        grad_out,
        flops=2 * owners * width * rows * count + 2 * depth * count * hidden,
        limit=8,
    )
    looked = exchange(looked, "hidden")

    made = run(
        products_body,
        S((members, piece + (chunks + 1) * SUBLANES, LANES), BF16),
        looked,
        grad_out,
        digits,
        flops=2 * depth * count * hidden,
        limit=8,
    )
    made = exchange(made, "vocab", groups)

    summed = run(
        group_sums,
        S((owners, piece + SUBLANES, LANES), BF16),
        made,
        flops=2 * members * count * owners * SUBLANES * LANES,
        limit=8,
    )
    summed = exchange(summed, "vocab")

    table_grad, projection_grad = run(
        last_sums, (S((width, rows), F32), S((depth, hidden), F32)), summed, flops=summed.size, limit=8
    )
    return table_grad.T, projection_grad


def solution(mesh):
    placed = (P("vocab"), P("vocab", None), P(None, "hidden"), P("vocab", "hidden"))
    return jax.shard_map(
        on_device,
        mesh=mesh,
        in_specs=placed,
        out_specs=(P("vocab", "hidden"), P(None, "hidden")),
        check_vma=False,
    )
```

```python
import jax
import jax.numpy as jnp
from jax import lax
from jax.experimental import pallas as pl
from jax.experimental.pallas import tpu as pltpu
from jax.sharding import PartitionSpec as P

F32, BF16, I32 = jnp.float32, jnp.bfloat16, jnp.int32
LANES, SUBLANES = 128, 8
ALONG_Y = 8


def run(body, out, *args, flops, limit, space=pltpu.VMEM, scratch=()):
    size = lambda a: a.size * a.dtype.itemsize
    vmem = pl.BlockSpec(memory_space=pltpu.VMEM)
    outs = jax.tree.leaves(out)
    if space != pltpu.VMEM:
        args = [pltpu.with_memory_space_constraint(a, space) for a in args]
    return pl.pallas_call(
        body,
        out_shape=out,
        in_specs=[pl.BlockSpec(memory_space=space)] * len(args),
        out_specs=jax.tree.map(lambda _: vmem, out),
        scratch_shapes=scratch,
        compiler_params=pltpu.CompilerParams(vmem_limit_bytes=limit * 2**20),
        cost_estimate=pl.CostEstimate(
            flops=flops, bytes_accessed=sum(map(size, [*args, *outs])), transcendentals=0
        ),
    )(*args)


def exchange(blocks, axis, groups=None):
    return lax.all_to_all(blocks, axis, split_axis=0, concat_axis=0, tiled=True, axis_index_groups=groups)


def contract_last(a, b):
    return lax.dot_general(a, b, (((1,), (1,)), ((), ())), preferred_element_type=F32)


def one_hot_rows(which, rows):
    shape = (rows, which.shape[1])
    return (lax.broadcasted_iota(I32, shape, 0) == which).astype(F32).astype(BF16)


def owner_and_row(token, rows):
    owner = ((token >> 6) * 4370) >> 16
    return owner, token - owner * rows


def columns_body(table_there, ids_there, out, places, digits, table, ids, arrivals):
    copies = [
        pltpu.make_async_copy(table_there, table, arrivals.at[0]),
        pltpu.make_async_copy(ids_there, ids, arrivals.at[1]),
    ]
    for copy in copies:
        copy.start()
    copies[1].wait()
    owner, row = owner_and_row(ids[...], table.shape[0])
    digits[...] = jnp.concatenate([owner * 8 + (row >> 7), row & 127], axis=0).astype(F32)
    for c in range(ids.shape[0]):
        at = slice(c * LANES, (c + 1) * LANES)
        places[0:1, at] = owner[c : c + 1]
        places[1:2, at] = row[c : c + 1]
    copies[0].wait()
    width = out.shape[1] * 2
    first = lax.axis_index("hidden") * width
    shape = (width, table.shape[1])
    lane = lax.broadcasted_iota(I32, shape, 1)
    pick = (lane == lax.broadcasted_iota(I32, shape, 0) + first).astype(F32).astype(BF16)
    mine = contract_last(pick, table[...])
    half, whole = width // 2, table.shape[0] // LANES * LANES
    mine = jnp.concatenate(
        [mine[:half, :whole], mine[half:, :whole], mine[:half, whole:], mine[half:, whole:]], axis=1
    ).astype(BF16)
    for peer in range(out.shape[0]):
        out[peer] = mine


def lookup_body(owners, table, places, projection, grad_out, out):
    width = out.shape[1] // 2
    count = places.shape[1]
    partial = contract_last(projection[...], grad_out[...])
    owner, row = places[0:1, :], places[1:2, :]
    half = width // 2
    lines = table.shape[2]
    rows = lines // 2
    whole = rows // LANES * LANES
    held = table[...].reshape(owners * half, lines)
    both = jnp.concatenate([held[:, :whole], held[:, whole : 2 * whole]], axis=0)
    every = jnp.dot(both, one_hot_rows(row, whole), preferred_element_type=F32)
    rest = held[:, 2 * whole :]
    left = row - whole
    right = jnp.where(left >= 0, left + (rows - whole), -1)
    tails = [one_hot_rows(left, LANES // 2), one_hot_rows(right, LANES)]
    tails[0] = jnp.concatenate([tails[0], jnp.zeros_like(tails[0])], axis=0)
    first = every[: owners * half] + jnp.dot(rest, tails[0], preferred_element_type=F32)
    other = every[owners * half :] + jnp.dot(rest, tails[1], preferred_element_type=F32)
    pair = owner - (lax.broadcasted_iota(I32, (width, count), 0) >= half).astype(I32)
    sums = []
    for found in (first, other):
        total = jnp.zeros((width, count), F32)
        for v in range(0, owners, 2):
            total = jnp.where(pair == v, found[v * half : (v + 2) * half], total)
        sums.append(total[:half] + total[half:])
    total = jnp.concatenate(sums, axis=0)
    mine = total.astype(BF16)
    for peer in range(out.shape[0]):
        out[peer, :width] = mine
        out[peer, width:] = partial[peer * width : (peer + 1) * width].astype(BF16)


def rows_of_lanes(value):
    return [value[:, j : j + LANES] for j in range(0, value.shape[1], LANES)]


def products_body(arrived, grad_out, digits, out):
    peers = arrived.shape[0]
    width = arrived.shape[1] // 2
    embedded = jnp.concatenate([arrived[p, :width] for p in range(peers)], axis=0)
    product = jnp.dot(embedded, grad_out[...], preferred_element_type=F32)
    product = jnp.concatenate(rows_of_lanes(product), axis=0).astype(BF16)
    grad = arrived[0, width:].astype(F32)
    for peer in range(1, peers):
        grad = grad + arrived[peer, width:].astype(F32)
    small = [part.astype(BF16) for part in [*rows_of_lanes(grad), digits[...]]]
    members = out.shape[0]
    piece = product.shape[0] // members
    for peer in range(members):
        out[peer, :piece] = product[peer * piece : (peer + 1) * piece]
        for c, part in enumerate(small):
            at = piece + c * SUBLANES
            out[peer, at : at + SUBLANES] = part


def group_sums_body(piece, arrived, out):
    members, owners = arrived.shape[0], out.shape[0]
    chunks = (arrived.shape[1] - piece) // SUBLANES - 1
    vocab = lax.axis_index("vocab")
    member = (vocab // ALONG_Y) * 2 + (vocab & 1)

    total = arrived[0, :piece].astype(F32)
    for peer in range(1, members):
        total = total + arrived[peer, :piece].astype(F32)
    total = total.astype(BF16)

    sums = jnp.zeros((owners * SUBLANES, LANES), F32)
    for peer in range(members):
        at = piece + chunks * SUBLANES
        digits = arrived[peer, at : at + SUBLANES].astype(F32).astype(I32)
        high, low = digits[:chunks], digits[chunks:]
        owner = jnp.where((high & 7) == member, high >> 3, -1)
        left, right = [], []
        for c in range(chunks):
            start = piece + c * SUBLANES
            part = arrived[peer, start : start + SUBLANES].astype(F32)
            owner_c = jnp.broadcast_to(owner[c : c + 1], part.shape)
            left.append(
                jnp.concatenate([jnp.where(owner_c == v, part, 0.0) for v in range(owners)], axis=0).astype(BF16)
            )
            right.append(one_hot_rows(low[c : c + 1], LANES))
        sums = sums + contract_last(jnp.concatenate(left, axis=1), jnp.concatenate(right, axis=1))
    sums = sums.astype(BF16)
    for v in range(owners):
        out[v, :piece] = total
        out[v, piece:] = sums[v * SUBLANES : (v + 1) * SUBLANES]


def last_sums_body(piece, arrived, table_grad, projection_grad):
    owners = arrived.shape[0]
    depth = projection_grad.shape[0]
    rows = table_grad.shape[1]
    members = depth * projection_grad.shape[1] // LANES // piece
    for member in range(members):
        first = (member >> 1) * ALONG_Y + (member & 1)
        total = arrived[first].astype(F32)
        for peer in range(first + 2, first + ALONG_Y, 2):
            total = total + arrived[peer].astype(F32)
        at, lane = member * piece % depth, member * piece // depth * LANES
        projection_grad[at : at + piece, lane : lane + LANES] = total[:piece]
        wide = min(LANES, rows - member * LANES)
        table_grad[:, member * LANES : member * LANES + wide] = total[piece:, :wide]


def on_device(token_ids, table, projection, grad_out):
    owners, peers = lax.axis_size("vocab"), lax.axis_size("hidden")
    along_x = owners // ALONG_Y
    members = 2 * along_x
    groups = [
        [x * ALONG_Y + y + bit for x in range(along_x) for bit in range(2)] for y in range(0, ALONG_Y, 2)
    ]
    rows, depth = table.shape
    width = depth // peers
    count = token_ids.shape[0]
    hidden = projection.shape[1]
    piece = depth * hidden // LANES // members
    chunks = count // LANES
    S = jax.ShapeDtypeStruct

    by_lane = token_ids.reshape(chunks, LANES)
    columns, places, digits = run(
        columns_body,
        (S((owners, width // 2, 2 * rows), BF16), S((2, count), I32), S((2 * chunks, LANES), F32)),
        table,
        by_lane,
        flops=2 * depth * rows * width,
        limit=4,
        space=pltpu.HBM,
        scratch=[
            pltpu.VMEM(table.shape, table.dtype),
            pltpu.VMEM(by_lane.shape, I32),
            pltpu.SemaphoreType.DMA((2,)),
        ],
    )
    columns = exchange(columns, "vocab")

    def lookup(*refs):
        lookup_body(owners, *refs)

    def group_sums(*refs):
        group_sums_body(piece, *refs)

    def last_sums(*refs):
        last_sums_body(piece, *refs)

    looked = run(
        lookup,
        S((peers, 2 * width, count), BF16),
        columns,
        places,
        projection,
        grad_out,
        flops=2 * owners * width * rows * count + 2 * depth * count * hidden,
        limit=8,
    )
    looked = exchange(looked, "hidden")

    made = run(
        products_body,
        S((members, piece + (chunks + 1) * SUBLANES, LANES), BF16),
        looked,
        grad_out,
        digits,
        flops=2 * depth * count * hidden,
        limit=8,
    )
    made = exchange(made, "vocab", groups)

    summed = run(
        group_sums,
        S((owners, piece + SUBLANES, LANES), BF16),
        made,
        flops=2 * members * count * owners * SUBLANES * LANES,
        limit=8,
    )
    summed = exchange(summed, "vocab")

    table_grad, projection_grad = run(
        last_sums, (S((width, rows), F32), S((depth, hidden), F32)), summed, flops=summed.size, limit=8
    )
    return table_grad.T, projection_grad


def solution(mesh):
    placed = (P("vocab"), P("vocab", None), P(None, "hidden"), P("vocab", "hidden"))
    return jax.shard_map(
        on_device,
        mesh=mesh,
        in_specs=placed,
        out_specs=(P("vocab", "hidden"), P(None, "hidden")),
        check_vma=False,
    )
```

```python
import jax
import jax.numpy as jnp
from jax import lax
from jax.experimental import pallas as pl
from jax.experimental.pallas import tpu as pltpu
from jax.sharding import PartitionSpec as P

F32, BF16, I32 = jnp.float32, jnp.bfloat16, jnp.int32
LANES, SUBLANES = 128, 8
ALONG_Y = 8


def run(body, out, *args, flops, limit, space=pltpu.VMEM, scratch=()):
    size = lambda a: a.size * a.dtype.itemsize
    vmem = pl.BlockSpec(memory_space=pltpu.VMEM)
    outs = jax.tree.leaves(out)
    if space != pltpu.VMEM:
        args = [pltpu.with_memory_space_constraint(a, space) for a in args]
    return pl.pallas_call(
        body,
        out_shape=out,
        in_specs=[pl.BlockSpec(memory_space=space)] * len(args),
        out_specs=jax.tree.map(lambda _: vmem, out),
        scratch_shapes=scratch,
        compiler_params=pltpu.CompilerParams(vmem_limit_bytes=limit * 2**20),
        cost_estimate=pl.CostEstimate(
            flops=flops, bytes_accessed=sum(map(size, [*args, *outs])), transcendentals=0
        ),
    )(*args)


def exchange(blocks, axis, groups=None):
    return lax.all_to_all(blocks, axis, split_axis=0, concat_axis=0, tiled=True, axis_index_groups=groups)


def contract_last(a, b):
    return lax.dot_general(a, b, (((1,), (1,)), ((), ())), preferred_element_type=F32)


def one_hot_rows(which, rows):
    shape = (rows, which.shape[1])
    return (lax.broadcasted_iota(I32, shape, 0) == which).astype(F32).astype(BF16)


def owner_and_row(token, rows):
    owner = ((token >> 6) * 4370) >> 16
    return owner, token - owner * rows


def columns_body(table_there, ids_there, out, places, digits, table, ids, arrivals):
    copies = [
        pltpu.make_async_copy(table_there, table, arrivals.at[0]),
        pltpu.make_async_copy(ids_there, ids, arrivals.at[1]),
    ]
    for copy in copies:
        copy.start()
    copies[1].wait()
    owner, row = owner_and_row(ids[...], table.shape[0])
    digits[...] = jnp.concatenate([owner * 8 + (row >> 7), row & 127], axis=0).astype(F32)
    for c in range(ids.shape[0]):
        at = slice(c * LANES, (c + 1) * LANES)
        places[0:1, at] = owner[c : c + 1]
        places[1:2, at] = row[c : c + 1]
    copies[0].wait()
    width = out.shape[1] * 2
    first = lax.axis_index("hidden") * width
    shape = (width, table.shape[1])
    lane = lax.broadcasted_iota(I32, shape, 1)
    pick = (lane == lax.broadcasted_iota(I32, shape, 0) + first).astype(F32).astype(BF16)
    mine = contract_last(pick, table[...])
    half, whole = width // 2, table.shape[0] // LANES * LANES
    mine = jnp.concatenate(
        [mine[:half, :whole], mine[half:, :whole], mine[:half, whole:], mine[half:, whole:]], axis=1
    ).astype(BF16)
    for peer in range(out.shape[0]):
        out[peer] = mine


def split_lanes(value, upper, keep, send):
    half = value.shape[1] // 2
    low, high = value[:, :half], value[:, half:]
    keep[...] = jnp.where(upper, high, low)
    send[...] = jnp.where(upper, low, high).astype(BF16)


def partial_body(projection, grad_out, keep, send):
    upper = (lax.axis_index("hidden") & 1) == 1
    split_lanes(contract_last(projection[...], grad_out[...]), upper, keep, send)


def pair_body(kept, arrived, keep, send):
    upper = ((lax.axis_index("hidden") >> 1) & 1) == 1
    split_lanes(kept[...] + arrived[...].astype(F32), upper, keep, send)


def lookup_body(owners, table, places, kept, arrived, out):
    width = out.shape[1]
    count = places.shape[1]
    partial = kept[...] + arrived[...].astype(F32)
    owner, row = places[0:1, :], places[1:2, :]
    half = width // 2
    lines = table.shape[2]
    rows = lines // 2
    whole = rows // LANES * LANES
    held = table[...].reshape(owners * half, lines)
    both = jnp.concatenate([held[:, :whole], held[:, whole : 2 * whole]], axis=0)
    every = jnp.dot(both, one_hot_rows(row, whole), preferred_element_type=F32)
    rest = held[:, 2 * whole :]
    left = row - whole
    right = jnp.where(left >= 0, left + (rows - whole), -1)
    tails = [one_hot_rows(left, LANES // 2), one_hot_rows(right, LANES)]
    tails[0] = jnp.concatenate([tails[0], jnp.zeros_like(tails[0])], axis=0)
    first = every[: owners * half] + jnp.dot(rest, tails[0], preferred_element_type=F32)
    other = every[owners * half :] + jnp.dot(rest, tails[1], preferred_element_type=F32)
    pair = owner - (lax.broadcasted_iota(I32, (width, count), 0) >= half).astype(I32)
    sums = []
    for found in (first, other):
        total = jnp.zeros((width, count), F32)
        for v in range(0, owners, 2):
            total = jnp.where(pair == v, found[v * half : (v + 2) * half], total)
        sums.append(total[:half] + total[half:])
    total = jnp.concatenate(sums, axis=0)
    mine = total.astype(BF16)
    for peer in range(out.shape[0]):
        out[peer, :, :count] = mine
        out[peer, :, count:] = partial[peer * width : (peer + 1) * width].astype(BF16)


def rows_of_lanes(value):
    return [value[:, j : j + LANES] for j in range(0, value.shape[1], LANES)]


def products_body(arrived, grad_out, digits, out):
    peers = arrived.shape[0]
    count = grad_out.shape[0]
    embedded = jnp.concatenate([arrived[p, :, :count] for p in range(peers)], axis=0)
    product = jnp.dot(embedded, grad_out[...], preferred_element_type=F32)
    product = jnp.concatenate(rows_of_lanes(product), axis=0).astype(BF16)
    grads = []
    for core in range(2):
        for chip in range(2):
            senders = range(2 * chip + core, peers, 4)
            grads.append(sum(arrived[p, :, count:].astype(F32) for p in senders))
    small = [part.astype(BF16) for part in [*grads, digits[...]]]
    members = out.shape[0]
    piece = product.shape[0] // members
    for peer in range(members):
        out[peer, :piece] = product[peer * piece : (peer + 1) * piece]
        for c, part in enumerate(small):
            at = piece + c * SUBLANES
            out[peer, at : at + SUBLANES] = part


def group_sums_body(piece, arrived, out):
    members, owners = arrived.shape[0], out.shape[0]
    chunks = (arrived.shape[1] - piece) // SUBLANES - 1
    vocab = lax.axis_index("vocab")
    member = (vocab // ALONG_Y) * 2 + (vocab & 1)

    total = arrived[0, :piece].astype(F32)
    for peer in range(1, members):
        total = total + arrived[peer, :piece].astype(F32)
    total = total.astype(BF16)

    sums = jnp.zeros((owners * SUBLANES, LANES), F32)
    for peer in range(members):
        at = piece + chunks * SUBLANES
        digits = arrived[peer, at : at + SUBLANES].astype(F32).astype(I32)
        high, low = digits[:chunks], digits[chunks:]
        owner = jnp.where((high & 7) == member, high >> 3, -1)
        left, right = [], []
        for c in range(chunks):
            start = piece + c * SUBLANES
            part = arrived[peer, start : start + SUBLANES].astype(F32)
            owner_c = jnp.broadcast_to(owner[c : c + 1], part.shape)
            left.append(
                jnp.concatenate([jnp.where(owner_c == v, part, 0.0) for v in range(owners)], axis=0).astype(BF16)
            )
            right.append(one_hot_rows(low[c : c + 1], LANES))
        sums = sums + contract_last(jnp.concatenate(left, axis=1), jnp.concatenate(right, axis=1))
    sums = sums.astype(BF16)
    for v in range(owners):
        out[v, :piece] = total
        out[v, piece:] = sums[v * SUBLANES : (v + 1) * SUBLANES]


def last_sums_body(piece, arrived, table_grad, projection_grad):
    owners = arrived.shape[0]
    depth = projection_grad.shape[0]
    rows = table_grad.shape[1]
    members = depth * projection_grad.shape[1] // LANES // piece
    for member in range(members):
        first = (member >> 1) * ALONG_Y + (member & 1)
        total = arrived[first].astype(F32)
        for peer in range(first + 2, first + ALONG_Y, 2):
            total = total + arrived[peer].astype(F32)
        at, lane = member * piece % depth, member * piece // depth * LANES
        projection_grad[at : at + piece, lane : lane + LANES] = total[:piece]
        wide = min(LANES, rows - member * LANES)
        table_grad[:, member * LANES : member * LANES + wide] = total[piece:, :wide]


def on_device(token_ids, table, projection, grad_out):
    owners, peers = lax.axis_size("vocab"), lax.axis_size("hidden")
    along_x = owners // ALONG_Y
    members = 2 * along_x
    groups = [
        [x * ALONG_Y + y + bit for x in range(along_x) for bit in range(2)] for y in range(0, ALONG_Y, 2)
    ]
    rows, depth = table.shape
    width = depth // peers
    count = token_ids.shape[0]
    hidden = projection.shape[1]
    piece = depth * hidden // LANES // members
    chunks = count // LANES
    S = jax.ShapeDtypeStruct

    by_lane = token_ids.reshape(chunks, LANES)
    columns, places, digits = run(
        columns_body,
        (S((owners, width // 2, 2 * rows), BF16), S((2, count), I32), S((2 * chunks, LANES), F32)),
        table,
        by_lane,
        flops=2 * depth * rows * width,
        limit=4,
        space=pltpu.HBM,
        scratch=[
            pltpu.VMEM(table.shape, table.dtype),
            pltpu.VMEM(by_lane.shape, I32),
            pltpu.SemaphoreType.DMA((2,)),
        ],
    )
    columns = exchange(columns, "vocab")

    def lookup(*refs):
        lookup_body(owners, *refs)

    def group_sums(*refs):
        group_sums_body(piece, *refs)

    def last_sums(*refs):
        last_sums_body(piece, *refs)

    def to_partner(send, bit):
        return lax.ppermute(send, "hidden", [(i, i ^ bit) for i in range(peers)])

    def halves(columns):
        return (S((depth, columns), F32), S((depth, columns), BF16))

    keep, send = run(
        partial_body, halves(count // 2), projection, grad_out, flops=2 * depth * count * hidden, limit=4
    )
    keep, send = run(pair_body, halves(count // 4), keep, to_partner(send, 1), flops=keep.size, limit=4)
    looked = run(
        lookup,
        S((peers, width, count + count // 4), BF16),
        columns,
        places,
        keep,
        to_partner(send, 2),
        flops=2 * owners * width * rows * count,
        limit=8,
    )
    looked = exchange(looked, "hidden")

    made = run(
        products_body,
        S((members, piece + (chunks + 1) * SUBLANES, LANES), BF16),
        looked,
        grad_out,
        digits,
        flops=2 * depth * count * hidden,
        limit=8,
    )
    made = exchange(made, "vocab", groups)

    summed = run(
        group_sums,
        S((owners, piece + SUBLANES, LANES), BF16),
        made,
        flops=2 * members * count * owners * SUBLANES * LANES,
        limit=8,
    )
    summed = exchange(summed, "vocab")

    table_grad, projection_grad = run(
        last_sums, (S((width, rows), F32), S((depth, hidden), F32)), summed, flops=summed.size, limit=8
    )
    return table_grad.T, projection_grad


def solution(mesh):
    placed = (P("vocab"), P("vocab", None), P(None, "hidden"), P("vocab", "hidden"))
    return jax.shard_map(
        on_device,
        mesh=mesh,
        in_specs=placed,
        out_specs=(P("vocab", "hidden"), P(None, "hidden")),
        check_vma=False,
    )
```

```python
import jax
import jax.numpy as jnp
from jax import lax
from jax.experimental import pallas as pl
from jax.experimental.pallas import tpu as pltpu
from jax.sharding import PartitionSpec as P

F32, BF16, I32 = jnp.float32, jnp.bfloat16, jnp.int32
LANES, SUBLANES = 128, 8
AT_ONCE = 8
ALONG_Y = 8


def run(body, out, *args, flops, limit, space=pltpu.VMEM, scratch=(), specs=None):
    size = lambda a: a.size * a.dtype.itemsize
    vmem = pl.BlockSpec(memory_space=pltpu.VMEM)
    outs = jax.tree.leaves(out)
    if space != pltpu.VMEM:
        args = [pltpu.with_memory_space_constraint(a, space) for a in args]
    return pl.pallas_call(
        body,
        out_shape=out,
        in_specs=[pl.BlockSpec(memory_space=space)] * len(args),
        out_specs=specs or jax.tree.map(lambda _: vmem, out),
        scratch_shapes=scratch,
        compiler_params=pltpu.CompilerParams(vmem_limit_bytes=limit * 2**20),
        cost_estimate=pl.CostEstimate(
            flops=flops, bytes_accessed=sum(map(size, [*args, *outs])), transcendentals=0
        ),
    )(*args)


def exchange(blocks, axis, groups=None):
    return lax.all_to_all(blocks, axis, split_axis=0, concat_axis=0, tiled=True, axis_index_groups=groups)


def contract_last(a, b):
    return lax.dot_general(a, b, (((1,), (1,)), ((), ())), preferred_element_type=F32)


def one_hot_rows(which, rows):
    shape = (rows, which.shape[1])
    return (lax.broadcasted_iota(I32, shape, 0) == which).astype(F32).astype(BF16)


def owner_and_row(token, rows):
    owner = ((token >> 6) * 4370) >> 16
    return owner, token - owner * rows


def columns_body(table_there, ids_there, out, places, digits, table, ids, copied, arrivals):
    copies = [
        pltpu.make_async_copy(table_there, table, arrivals.at[0]),
        pltpu.make_async_copy(ids_there, ids, arrivals.at[1]),
    ]
    for copy in copies:
        copy.start()
    copies[0].wait()
    width = copied.shape[1] * 2
    first = lax.axis_index("hidden") * width
    shape = (width, table.shape[1])
    lane = lax.broadcasted_iota(I32, shape, 1)
    pick = (lane == lax.broadcasted_iota(I32, shape, 0) + first).astype(F32).astype(BF16)
    mine = contract_last(pick, table[...])
    half, whole = width // 2, table.shape[0] // LANES * LANES
    mine = jnp.concatenate(
        [mine[:half, :whole], mine[half:, :whole], mine[:half, whole:], mine[half:, whole:]], axis=1
    ).astype(BF16)
    at_once = copied.shape[0]
    for peer in range(at_once):
        copied[peer] = mine
    copies[1].wait()
    owner, row = owner_and_row(ids[...], table.shape[0])
    digits[...] = jnp.concatenate([owner * 8 + (row >> 7), row & 127], axis=0).astype(F32)
    for c in range(ids.shape[0]):
        at = slice(c * LANES, (c + 1) * LANES)
        places[0:1, at] = owner[c : c + 1]
        places[1:2, at] = row[c : c + 1]
    leaving = [
        pltpu.make_async_copy(copied, out.at[pl.ds(i * at_once, at_once)], arrivals.at[2 + i])
        for i in range(out.shape[0] // at_once)
    ]
    for copy in leaving:
        copy.start()
    for copy in leaving:
        copy.wait()


def split_lanes(value, upper, keep, send):
    half = value.shape[1] // 2
    low, high = value[:, :half], value[:, half:]
    keep[...] = jnp.where(upper, high, low)
    send[...] = jnp.where(upper, low, high).astype(BF16)


def partial_body(projection, grad_out, keep, send):
    upper = (lax.axis_index("hidden") & 1) == 1
    split_lanes(contract_last(projection[...], grad_out[...]), upper, keep, send)


def pair_body(kept, arrived, keep, send):
    upper = ((lax.axis_index("hidden") >> 1) & 1) == 1
    split_lanes(kept[...] + arrived[...].astype(F32), upper, keep, send)


def lookup_body(owners, table, places, kept, arrived, out):
    width = out.shape[1]
    count = places.shape[1]
    partial = kept[...] + arrived[...].astype(F32)
    owner, row = places[0:1, :], places[1:2, :]
    half = width // 2
    lines = table.shape[2]
    rows = lines // 2
    whole = rows // LANES * LANES
    held = table[...].reshape(owners * half, lines)
    both = jnp.concatenate([held[:, :whole], held[:, whole : 2 * whole]], axis=0)
    every = jnp.dot(both, one_hot_rows(row, whole), preferred_element_type=F32)
    rest = held[:, 2 * whole :]
    left = row - whole
    right = jnp.where(left >= 0, left + (rows - whole), -1)
    tails = [one_hot_rows(left, LANES // 2), one_hot_rows(right, LANES)]
    tails[0] = jnp.concatenate([tails[0], jnp.zeros_like(tails[0])], axis=0)
    first = every[: owners * half] + jnp.dot(rest, tails[0], preferred_element_type=F32)
    other = every[owners * half :] + jnp.dot(rest, tails[1], preferred_element_type=F32)
    pair = owner - (lax.broadcasted_iota(I32, (width, count), 0) >= half).astype(I32)
    sums = []
    for found in (first, other):
        total = jnp.zeros((width, count), F32)
        for v in range(0, owners, 2):
            total = jnp.where(pair == v, found[v * half : (v + 2) * half], total)
        sums.append(total[:half] + total[half:])
    total = jnp.concatenate(sums, axis=0)
    mine = total.astype(BF16)
    for peer in range(out.shape[0]):
        out[peer, :, :count] = mine
        out[peer, :, count:] = partial[peer * width : (peer + 1) * width].astype(BF16)


def rows_of_lanes(value):
    return [value[:, j : j + LANES] for j in range(0, value.shape[1], LANES)]


def products_body(arrived, grad_out, digits, out):
    peers = arrived.shape[0]
    count = grad_out.shape[0]
    embedded = jnp.concatenate([arrived[p, :, :count] for p in range(peers)], axis=0)
    product = jnp.dot(embedded, grad_out[...], preferred_element_type=F32)
    product = jnp.concatenate(rows_of_lanes(product), axis=0).astype(BF16)
    grads = []
    for core in range(2):
        for chip in range(2):
            senders = range(2 * chip + core, peers, 4)
            grads.append(sum(arrived[p, :, count:].astype(F32) for p in senders))
    small = [part.astype(BF16) for part in [*grads, digits[...]]]
    members = out.shape[0]
    piece = product.shape[0] // members
    for peer in range(members):
        out[peer, :piece] = product[peer * piece : (peer + 1) * piece]
        for c, part in enumerate(small):
            at = piece + c * SUBLANES
            out[peer, at : at + SUBLANES] = part


def group_sums_body(piece, arrived, out):
    members, owners = arrived.shape[0], out.shape[0]
    chunks = (arrived.shape[1] - piece) // SUBLANES - 1
    vocab = lax.axis_index("vocab")
    member = (vocab // ALONG_Y) * 2 + (vocab & 1)

    total = arrived[0, :piece].astype(F32)
    for peer in range(1, members):
        total = total + arrived[peer, :piece].astype(F32)
    total = total.astype(BF16)

    sums = jnp.zeros((owners * SUBLANES, LANES), F32)
    for peer in range(members):
        at = piece + chunks * SUBLANES
        digits = arrived[peer, at : at + SUBLANES].astype(F32).astype(I32)
        high, low = digits[:chunks], digits[chunks:]
        owner = jnp.where((high & 7) == member, high >> 3, -1)
        left, right = [], []
        for c in range(chunks):
            start = piece + c * SUBLANES
            part = arrived[peer, start : start + SUBLANES].astype(F32)
            owner_c = jnp.broadcast_to(owner[c : c + 1], part.shape)
            left.append(
                jnp.concatenate([jnp.where(owner_c == v, part, 0.0) for v in range(owners)], axis=0).astype(BF16)
            )
            right.append(one_hot_rows(low[c : c + 1], LANES))
        sums = sums + contract_last(jnp.concatenate(left, axis=1), jnp.concatenate(right, axis=1))
    sums = sums.astype(BF16)
    for v in range(owners):
        out[v, :piece] = total
        out[v, piece:] = sums[v * SUBLANES : (v + 1) * SUBLANES]


def last_sums_body(piece, arrived, table_grad, projection_grad):
    owners = arrived.shape[0]
    depth = projection_grad.shape[0]
    rows = table_grad.shape[1]
    members = depth * projection_grad.shape[1] // LANES // piece
    for member in range(members):
        first = (member >> 1) * ALONG_Y + (member & 1)
        total = arrived[first].astype(F32)
        for peer in range(first + 2, first + ALONG_Y, 2):
            total = total + arrived[peer].astype(F32)
        at, lane = member * piece % depth, member * piece // depth * LANES
        projection_grad[at : at + piece, lane : lane + LANES] = total[:piece]
        wide = min(LANES, rows - member * LANES)
        table_grad[:, member * LANES : member * LANES + wide] = total[piece:, :wide]


def on_device(token_ids, table, projection, grad_out):
    owners, peers = lax.axis_size("vocab"), lax.axis_size("hidden")
    along_x = owners // ALONG_Y
    members = 2 * along_x
    groups = [
        [x * ALONG_Y + y + bit for x in range(along_x) for bit in range(2)] for y in range(0, ALONG_Y, 2)
    ]
    rows, depth = table.shape
    width = depth // peers
    count = token_ids.shape[0]
    hidden = projection.shape[1]
    piece = depth * hidden // LANES // members
    chunks = count // LANES
    S = jax.ShapeDtypeStruct

    by_lane = token_ids.reshape(chunks, LANES)
    columns, places, digits = run(
        columns_body,
        (S((owners, width // 2, 2 * rows), BF16), S((2, count), I32), S((2 * chunks, LANES), F32)),
        table,
        by_lane,
        flops=2 * depth * rows * width,
        limit=4,
        space=pltpu.HBM,
        scratch=[
            pltpu.VMEM(table.shape, table.dtype),
            pltpu.VMEM(by_lane.shape, I32),
            pltpu.VMEM((AT_ONCE, width // 2, 2 * rows), BF16),
            pltpu.SemaphoreType.DMA((2 + owners // AT_ONCE,)),
        ],
        specs=tuple(pl.BlockSpec(memory_space=place) for place in (pltpu.HBM, pltpu.VMEM, pltpu.VMEM)),
    )
    columns = exchange(columns, "vocab")

    def lookup(*refs):
        lookup_body(owners, *refs)

    def group_sums(*refs):
        group_sums_body(piece, *refs)

    def last_sums(*refs):
        last_sums_body(piece, *refs)

    def to_partner(send, bit):
        return lax.ppermute(send, "hidden", [(i, i ^ bit) for i in range(peers)])

    def halves(columns):
        return (S((depth, columns), F32), S((depth, columns), BF16))

    keep, send = run(
        partial_body, halves(count // 2), projection, grad_out, flops=2 * depth * count * hidden, limit=4
    )
    keep, send = run(pair_body, halves(count // 4), keep, to_partner(send, 1), flops=keep.size, limit=4)
    looked = run(
        lookup,
        S((peers, width, count + count // 4), BF16),
        columns,
        places,
        keep,
        to_partner(send, 2),
        flops=2 * owners * width * rows * count,
        limit=8,
    )
    looked = exchange(looked, "hidden")

    made = run(
        products_body,
        S((members, piece + (chunks + 1) * SUBLANES, LANES), BF16),
        looked,
        grad_out,
        digits,
        flops=2 * depth * count * hidden,
        limit=8,
    )
    made = exchange(made, "vocab", groups)

    summed = run(
        group_sums,
        S((owners, piece + SUBLANES, LANES), BF16),
        made,
        flops=2 * members * count * owners * SUBLANES * LANES,
        limit=8,
    )
    summed = exchange(summed, "vocab")

    table_grad, projection_grad = run(
        last_sums, (S((width, rows), F32), S((depth, hidden), F32)), summed, flops=summed.size, limit=8
    )
    return table_grad.T, projection_grad


def solution(mesh):
    placed = (P("vocab"), P("vocab", None), P(None, "hidden"), P("vocab", "hidden"))
    return jax.shard_map(
        on_device,
        mesh=mesh,
        in_specs=placed,
        out_specs=(P("vocab", "hidden"), P(None, "hidden")),
        check_vma=False,
    )
```

```python
import jax
import jax.numpy as jnp
from jax import lax
from jax.experimental import pallas as pl
from jax.experimental.pallas import tpu as pltpu
from jax.sharding import PartitionSpec as P

F32, BF16, I32 = jnp.float32, jnp.bfloat16, jnp.int32
LANES, SUBLANES = 128, 8
AT_ONCE = 8
ALONG_Y = 8


def run(body, out, *args, flops, limit, space=pltpu.VMEM, scratch=(), specs=None):
    size = lambda a: a.size * a.dtype.itemsize
    vmem = pl.BlockSpec(memory_space=pltpu.VMEM)
    outs = jax.tree.leaves(out)
    if space != pltpu.VMEM:
        args = [pltpu.with_memory_space_constraint(a, space) for a in args]
    return pl.pallas_call(
        body,
        out_shape=out,
        in_specs=[pl.BlockSpec(memory_space=space)] * len(args),
        out_specs=specs or jax.tree.map(lambda _: vmem, out),
        scratch_shapes=scratch,
        compiler_params=pltpu.CompilerParams(vmem_limit_bytes=limit * 2**20),
        cost_estimate=pl.CostEstimate(
            flops=flops, bytes_accessed=sum(map(size, [*args, *outs])), transcendentals=0
        ),
    )(*args)


def exchange(blocks, axis, groups=None):
    return lax.all_to_all(blocks, axis, split_axis=0, concat_axis=0, tiled=True, axis_index_groups=groups)


def contract_last(a, b):
    return lax.dot_general(a, b, (((1,), (1,)), ((), ())), preferred_element_type=F32)


def one_hot_rows(which, rows):
    shape = (rows, which.shape[1])
    return (lax.broadcasted_iota(I32, shape, 0) == which).astype(F32).astype(BF16)


def turn(vocab, owners):
    return (vocab % ALONG_Y) * (owners // ALONG_Y) + vocab // ALONG_Y


def owner_and_row(token, rows):
    owner = ((token >> 6) * 4370) >> 16
    return owner, token - owner * rows


def columns_body(table_there, ids_there, out, places, digits, table, ids, copied, arrivals):
    copies = [
        pltpu.make_async_copy(table_there, table, arrivals.at[0]),
        pltpu.make_async_copy(ids_there, ids, arrivals.at[1]),
    ]
    for copy in copies:
        copy.start()
    copies[0].wait()
    width = copied.shape[1] * 2
    first = lax.axis_index("hidden") * width
    shape = (width, table.shape[1])
    lane = lax.broadcasted_iota(I32, shape, 1)
    pick = (lane == lax.broadcasted_iota(I32, shape, 0) + first).astype(F32).astype(BF16)
    mine = contract_last(pick, table[...])
    half, whole = width // 2, table.shape[0] // LANES * LANES
    mine = jnp.concatenate(
        [mine[:half, :whole], mine[half:, :whole], mine[:half, whole:], mine[half:, whole:]], axis=1
    ).astype(BF16)
    at_once = copied.shape[0]
    for peer in range(at_once):
        copied[peer] = mine
    copies[1].wait()
    along_x = out.shape[0] // ALONG_Y
    owner, row = owner_and_row(ids[...], table.shape[0])
    digits[...] = jnp.concatenate([owner * 8 + (row >> 7), row & 127], axis=0).astype(F32)
    for c in range(ids.shape[0]):
        at = slice(c * LANES, (c + 1) * LANES)
        places[0:1, at] = (owner[c : c + 1] & (ALONG_Y - 1)) * along_x + (owner[c : c + 1] >> 3)
        places[1:2, at] = row[c : c + 1]
    leaving = [
        pltpu.make_async_copy(copied, out.at[pl.ds(i * at_once, at_once)], arrivals.at[2 + i])
        for i in range(out.shape[0] // at_once)
    ]
    for copy in leaving:
        copy.start()
    for copy in leaving:
        copy.wait()


def split_lanes(value, upper, keep, send):
    half = value.shape[1] // 2
    low, high = value[:, :half], value[:, half:]
    keep[...] = jnp.where(upper, high, low)
    send[...] = jnp.where(upper, low, high).astype(BF16)


def partial_body(projection, grad_out, keep, send):
    upper = (lax.axis_index("hidden") & 1) == 1
    split_lanes(contract_last(projection[...], grad_out[...]), upper, keep, send)


def pair_body(kept, arrived, keep, send):
    upper = ((lax.axis_index("hidden") >> 1) & 1) == 1
    split_lanes(kept[...] + arrived[...].astype(F32), upper, keep, send)


def lookup_body(owners, table, places, kept, arrived, out):
    width = out.shape[1]
    count = places.shape[1]
    partial = kept[...] + arrived[...].astype(F32)
    owner, row = places[0:1, :], places[1:2, :]
    half = width // 2
    lines = table.shape[2]
    rows = lines // 2
    whole = rows // LANES * LANES
    held = table[...].reshape(owners * half, lines)
    both = jnp.concatenate([held[:, :whole], held[:, whole : 2 * whole]], axis=0)
    every = jnp.dot(both, one_hot_rows(row, whole), preferred_element_type=F32)
    rest = held[:, 2 * whole :]
    left = row - whole
    right = jnp.where(left >= 0, left + (rows - whole), -1)
    tails = [one_hot_rows(left, LANES // 2), one_hot_rows(right, LANES)]
    tails[0] = jnp.concatenate([tails[0], jnp.zeros_like(tails[0])], axis=0)
    first = every[: owners * half] + jnp.dot(rest, tails[0], preferred_element_type=F32)
    other = every[owners * half :] + jnp.dot(rest, tails[1], preferred_element_type=F32)
    pair = owner - (lax.broadcasted_iota(I32, (width, count), 0) >= half).astype(I32)
    sums = []
    for found in (first, other):
        total = jnp.zeros((width, count), F32)
        for v in range(0, owners, 2):
            total = jnp.where(pair == v, found[v * half : (v + 2) * half], total)
        sums.append(total[:half] + total[half:])
    total = jnp.concatenate(sums, axis=0)
    mine = total.astype(BF16)
    for peer in range(out.shape[0]):
        out[peer, :, :count] = mine
        out[peer, :, count:] = partial[peer * width : (peer + 1) * width].astype(BF16)


def rows_of_lanes(value):
    return [value[:, j : j + LANES] for j in range(0, value.shape[1], LANES)]


def products_body(arrived, grad_out, digits, out):
    peers = arrived.shape[0]
    count = grad_out.shape[0]
    embedded = jnp.concatenate([arrived[p, :, :count] for p in range(peers)], axis=0)
    product = jnp.dot(embedded, grad_out[...], preferred_element_type=F32)
    product = jnp.concatenate(rows_of_lanes(product), axis=0).astype(BF16)
    grads = []
    for core in range(2):
        for chip in range(2):
            senders = range(2 * chip + core, peers, 4)
            grads.append(sum(arrived[p, :, count:].astype(F32) for p in senders))
    small = [part.astype(BF16) for part in [*grads, digits[...]]]
    members = out.shape[0]
    piece = product.shape[0] // members
    for peer in range(members):
        out[peer, :piece] = product[peer * piece : (peer + 1) * piece]
        for c, part in enumerate(small):
            at = piece + c * SUBLANES
            out[peer, at : at + SUBLANES] = part


def group_sums_body(piece, arrived, out):
    members, owners = arrived.shape[0], out.shape[0]
    chunks = (arrived.shape[1] - piece) // SUBLANES - 1
    vocab = lax.axis_index("vocab")
    member = (vocab // ALONG_Y) * 2 + (vocab & 1)

    total = arrived[0, :piece].astype(F32)
    for peer in range(1, members):
        total = total + arrived[peer, :piece].astype(F32)
    total = total.astype(BF16)

    sums = jnp.zeros((owners * SUBLANES, LANES), F32)
    for peer in range(members):
        at = piece + chunks * SUBLANES
        digits = arrived[peer, at : at + SUBLANES].astype(F32).astype(I32)
        high, low = digits[:chunks], digits[chunks:]
        owner = jnp.where((high & 7) == member, high >> 3, -1)
        left, right = [], []
        for c in range(chunks):
            start = piece + c * SUBLANES
            part = arrived[peer, start : start + SUBLANES].astype(F32)
            owner_c = jnp.broadcast_to(owner[c : c + 1], part.shape)
            left.append(
                jnp.concatenate([jnp.where(owner_c == v, part, 0.0) for v in range(owners)], axis=0).astype(BF16)
            )
            right.append(one_hot_rows(low[c : c + 1], LANES))
        sums = sums + contract_last(jnp.concatenate(left, axis=1), jnp.concatenate(right, axis=1))
    sums = sums.astype(BF16)
    for v in range(owners):
        out[turn(v, owners), :piece] = total
        out[turn(v, owners), piece:] = sums[v * SUBLANES : (v + 1) * SUBLANES]


def last_sums_body(piece, arrived, table_grad, projection_grad):
    owners = arrived.shape[0]
    depth = projection_grad.shape[0]
    rows = table_grad.shape[1]
    members = depth * projection_grad.shape[1] // LANES // piece
    for member in range(members):
        first = (member >> 1) * ALONG_Y + (member & 1)
        total = arrived[turn(first, owners)].astype(F32)
        for peer in range(first + 2, first + ALONG_Y, 2):
            total = total + arrived[turn(peer, owners)].astype(F32)
        at, lane = member * piece % depth, member * piece // depth * LANES
        projection_grad[at : at + piece, lane : lane + LANES] = total[:piece]
        wide = min(LANES, rows - member * LANES)
        table_grad[:, member * LANES : member * LANES + wide] = total[piece:, :wide]


def on_device(token_ids, table, projection, grad_out):
    owners, peers = lax.axis_size("vocab"), lax.axis_size("hidden")
    along_x = owners // ALONG_Y
    members = 2 * along_x
    groups = [
        [x * ALONG_Y + y + bit for x in range(along_x) for bit in range(2)] for y in range(0, ALONG_Y, 2)
    ]
    turned = [sorted(range(owners), key=lambda v: turn(v, owners))]
    rows, depth = table.shape
    width = depth // peers
    count = token_ids.shape[0]
    hidden = projection.shape[1]
    piece = depth * hidden // LANES // members
    chunks = count // LANES
    S = jax.ShapeDtypeStruct

    by_lane = token_ids.reshape(chunks, LANES)
    columns, places, digits = run(
        columns_body,
        (S((owners, width // 2, 2 * rows), BF16), S((2, count), I32), S((2 * chunks, LANES), F32)),
        table,
        by_lane,
        flops=2 * depth * rows * width,
        limit=4,
        space=pltpu.HBM,
        scratch=[
            pltpu.VMEM(table.shape, table.dtype),
            pltpu.VMEM(by_lane.shape, I32),
            pltpu.VMEM((AT_ONCE, width // 2, 2 * rows), BF16),
            pltpu.SemaphoreType.DMA((2 + owners // AT_ONCE,)),
        ],
        specs=tuple(pl.BlockSpec(memory_space=place) for place in (pltpu.HBM, pltpu.VMEM, pltpu.VMEM)),
    )
    columns = exchange(columns, "vocab", turned)

    def lookup(*refs):
        lookup_body(owners, *refs)

    def group_sums(*refs):
        group_sums_body(piece, *refs)

    def last_sums(*refs):
        last_sums_body(piece, *refs)

    def to_partner(send, bit):
        return lax.ppermute(send, "hidden", [(i, i ^ bit) for i in range(peers)])

    def halves(columns):
        return (S((depth, columns), F32), S((depth, columns), BF16))

    keep, send = run(
        partial_body, halves(count // 2), projection, grad_out, flops=2 * depth * count * hidden, limit=4
    )
    keep, send = run(pair_body, halves(count // 4), keep, to_partner(send, 1), flops=keep.size, limit=4)
    looked = run(
        lookup,
        S((peers, width, count + count // 4), BF16),
        columns,
        places,
        keep,
        to_partner(send, 2),
        flops=2 * owners * width * rows * count,
        limit=8,
    )
    looked = exchange(looked, "hidden")

    made = run(
        products_body,
        S((members, piece + (chunks + 1) * SUBLANES, LANES), BF16),
        looked,
        grad_out,
        digits,
        flops=2 * depth * count * hidden,
        limit=8,
    )
    made = exchange(made, "vocab", groups)

    summed = run(
        group_sums,
        S((owners, piece + SUBLANES, LANES), BF16),
        made,
        flops=2 * members * count * owners * SUBLANES * LANES,
        limit=8,
    )
    summed = exchange(summed, "vocab", turned)

    table_grad, projection_grad = run(
        last_sums, (S((width, rows), F32), S((depth, hidden), F32)), summed, flops=summed.size, limit=8
    )
    return table_grad.T, projection_grad


def solution(mesh):
    placed = (P("vocab"), P("vocab", None), P(None, "hidden"), P("vocab", "hidden"))
    return jax.shard_map(
        on_device,
        mesh=mesh,
        in_specs=placed,
        out_specs=(P("vocab", "hidden"), P(None, "hidden")),
        check_vma=False,
    )
```

```python
import jax
import jax.numpy as jnp
from jax import lax
from jax.experimental import pallas as pl
from jax.experimental.pallas import tpu as pltpu
from jax.sharding import PartitionSpec as P

F32, BF16, I32 = jnp.float32, jnp.bfloat16, jnp.int32
LANES, SUBLANES = 128, 8
ALONG_Y = 8


def run(body, out, *args, flops, limit, space=pltpu.VMEM, scratch=()):
    size = lambda a: a.size * a.dtype.itemsize
    vmem = pl.BlockSpec(memory_space=pltpu.VMEM)
    outs = jax.tree.leaves(out)
    if space != pltpu.VMEM:
        args = [pltpu.with_memory_space_constraint(a, space) for a in args]
    return pl.pallas_call(
        body,
        out_shape=out,
        in_specs=[pl.BlockSpec(memory_space=space)] * len(args),
        out_specs=jax.tree.map(lambda _: vmem, out),
        scratch_shapes=scratch,
        compiler_params=pltpu.CompilerParams(vmem_limit_bytes=limit * 2**20),
        cost_estimate=pl.CostEstimate(
            flops=flops, bytes_accessed=sum(map(size, [*args, *outs])), transcendentals=0
        ),
    )(*args)


def exchange(blocks, axis, groups=None):
    return lax.all_to_all(blocks, axis, split_axis=0, concat_axis=0, tiled=True, axis_index_groups=groups)


def contract_last(a, b):
    return lax.dot_general(a, b, (((1,), (1,)), ((), ())), preferred_element_type=F32)


def one_hot_rows(which, rows):
    shape = (rows, which.shape[1])
    return (lax.broadcasted_iota(I32, shape, 0) == which).astype(F32).astype(BF16)


def owner_and_row(token, rows):
    owner = ((token >> 6) * 4370) >> 16
    return owner, token - owner * rows


def columns_body(table_there, out, table, arrival):
    copy = pltpu.make_async_copy(table_there, table, arrival.at[0])
    copy.start()
    copy.wait()
    width = out.shape[1] * 2
    first = lax.axis_index("hidden") * width
    shape = (width, table.shape[1])
    lane = lax.broadcasted_iota(I32, shape, 1)
    pick = (lane == lax.broadcasted_iota(I32, shape, 0) + first).astype(F32).astype(BF16)
    mine = contract_last(pick, table[...])
    half, whole = width // 2, table.shape[0] // LANES * LANES
    mine = jnp.concatenate(
        [mine[:half, :whole], mine[half:, :whole], mine[:half, whole:], mine[half:, whole:]], axis=1
    ).astype(BF16)
    for peer in range(out.shape[0]):
        out[peer] = mine


def split_lanes(value, upper, keep, send):
    half = value.shape[1] // 2
    low, high = value[:, :half], value[:, half:]
    keep[...] = jnp.where(upper, high, low)
    send[...] = jnp.where(upper, low, high).astype(BF16)


def partial_body(rows, projection, grad_out, ids, keep, send, places, digits):
    owner, row = owner_and_row(ids[...], rows)
    digits[...] = jnp.concatenate([owner * 8 + (row >> 7), row & 127], axis=0).astype(F32)
    for c in range(ids.shape[0]):
        at = slice(c * LANES, (c + 1) * LANES)
        places[0:1, at] = owner[c : c + 1]
        places[1:2, at] = row[c : c + 1]
    upper = (lax.axis_index("hidden") & 1) == 1
    split_lanes(contract_last(projection[...], grad_out[...]), upper, keep, send)


def pair_body(kept, arrived, keep, send):
    upper = ((lax.axis_index("hidden") >> 1) & 1) == 1
    split_lanes(kept[...] + arrived[...].astype(F32), upper, keep, send)


def lookup_body(owners, table, places, kept, arrived, out):
    width = out.shape[1]
    count = places.shape[1]
    partial = kept[...] + arrived[...].astype(F32)
    owner, row = places[0:1, :], places[1:2, :]
    half = width // 2
    lines = table.shape[2]
    rows = lines // 2
    whole = rows // LANES * LANES
    held = table[...].reshape(owners * half, lines)
    both = jnp.concatenate([held[:, :whole], held[:, whole : 2 * whole]], axis=0)
    every = jnp.dot(both, one_hot_rows(row, whole), preferred_element_type=F32)
    rest = held[:, 2 * whole :]
    left = row - whole
    right = jnp.where(left >= 0, left + (rows - whole), -1)
    left = jnp.where(left < rows - whole, left, -1)
    tails = jnp.concatenate([one_hot_rows(left, LANES), one_hot_rows(right, LANES)], axis=1)
    ends = jnp.dot(rest, tails, preferred_element_type=F32)
    first = every[: owners * half] + ends[:, :count]
    other = every[owners * half :] + ends[:, count:]
    pair = owner - (lax.broadcasted_iota(I32, (width, count), 0) >= half).astype(I32)
    sums = []
    for found in (first, other):
        total = jnp.zeros((width, count), F32)
        for v in range(0, owners, 2):
            total = jnp.where(pair == v, found[v * half : (v + 2) * half], total)
        sums.append(total[:half] + total[half:])
    total = jnp.concatenate(sums, axis=0)
    mine = total.astype(BF16)
    for peer in range(out.shape[0]):
        out[peer, :, :count] = mine
        out[peer, :, count:] = partial[peer * width : (peer + 1) * width].astype(BF16)


def rows_of_lanes(value):
    return [value[:, j : j + LANES] for j in range(0, value.shape[1], LANES)]


def products_body(arrived, grad_out, digits, out):
    peers = arrived.shape[0]
    count = grad_out.shape[0]
    embedded = jnp.concatenate([arrived[p, :, :count] for p in range(peers)], axis=0)
    product = jnp.dot(embedded, grad_out[...], preferred_element_type=F32)
    product = jnp.concatenate(rows_of_lanes(product), axis=0).astype(BF16)
    grads = []
    for core in range(2):
        for chip in range(2):
            senders = range(2 * chip + core, peers, 4)
            grads.append(sum(arrived[p, :, count:].astype(F32) for p in senders))
    small = [part.astype(BF16) for part in [*grads, digits[...]]]
    members = out.shape[0]
    piece = product.shape[0] // members
    for peer in range(members):
        out[peer, :piece] = product[peer * piece : (peer + 1) * piece]
        for c, part in enumerate(small):
            at = piece + c * SUBLANES
            out[peer, at : at + SUBLANES] = part


def group_sums_body(piece, arrived, out):
    members, owners = arrived.shape[0], out.shape[0]
    chunks = (arrived.shape[1] - piece) // SUBLANES - 1
    vocab = lax.axis_index("vocab")
    member = (vocab // ALONG_Y) * 2 + (vocab & 1)

    total = arrived[0, :piece].astype(F32)
    for peer in range(1, members):
        total = total + arrived[peer, :piece].astype(F32)
    total = total.astype(BF16)

    sums = jnp.zeros((owners * SUBLANES, LANES), F32)
    for peer in range(members):
        at = piece + chunks * SUBLANES
        digits = arrived[peer, at : at + SUBLANES].astype(F32).astype(I32)
        high, low = digits[:chunks], digits[chunks:]
        owner = jnp.where((high & 7) == member, high >> 3, -1)
        left, right = [], []
        for c in range(chunks):
            start = piece + c * SUBLANES
            part = arrived[peer, start : start + SUBLANES].astype(F32)
            owner_c = jnp.broadcast_to(owner[c : c + 1], part.shape)
            left.append(
                jnp.concatenate([jnp.where(owner_c == v, part, 0.0) for v in range(owners)], axis=0).astype(BF16)
            )
            right.append(one_hot_rows(low[c : c + 1], LANES))
        sums = sums + contract_last(jnp.concatenate(left, axis=1), jnp.concatenate(right, axis=1))
    sums = sums.astype(BF16)
    for v in range(owners):
        out[v, :piece] = total
        out[v, piece:] = sums[v * SUBLANES : (v + 1) * SUBLANES]


def last_sums_body(piece, arrived, table_grad, projection_grad):
    owners = arrived.shape[0]
    depth = projection_grad.shape[0]
    rows = table_grad.shape[1]
    members = depth * projection_grad.shape[1] // LANES // piece
    for member in range(members):
        first = (member >> 1) * ALONG_Y + (member & 1)
        total = arrived[first].astype(F32)
        for peer in range(first + 2, first + ALONG_Y, 2):
            total = total + arrived[peer].astype(F32)
        at, lane = member * piece % depth, member * piece // depth * LANES
        projection_grad[at : at + piece, lane : lane + LANES] = total[:piece]
        wide = min(LANES, rows - member * LANES)
        table_grad[:, member * LANES : member * LANES + wide] = total[piece:, :wide]


def on_device(token_ids, table, projection, grad_out):
    owners, peers = lax.axis_size("vocab"), lax.axis_size("hidden")
    along_x = owners // ALONG_Y
    members = 2 * along_x
    groups = [
        [x * ALONG_Y + y + bit for x in range(along_x) for bit in range(2)] for y in range(0, ALONG_Y, 2)
    ]
    rows, depth = table.shape
    width = depth // peers
    count = token_ids.shape[0]
    hidden = projection.shape[1]
    piece = depth * hidden // LANES // members
    chunks = count // LANES
    S = jax.ShapeDtypeStruct

    columns = run(
        columns_body,
        S((owners, width // 2, 2 * rows), BF16),
        table,
        flops=2 * depth * rows * width,
        limit=4,
        space=pltpu.HBM,
        scratch=[pltpu.VMEM(table.shape, table.dtype), pltpu.SemaphoreType.DMA((1,))],
    )
    columns = exchange(columns, "vocab")

    def lookup(*refs):
        lookup_body(owners, *refs)

    def group_sums(*refs):
        group_sums_body(piece, *refs)

    def last_sums(*refs):
        last_sums_body(piece, *refs)

    def to_partner(send, bit):
        return lax.ppermute(send, "hidden", [(i, i ^ bit) for i in range(peers)])

    def halves(columns):
        return (S((depth, columns), F32), S((depth, columns), BF16))

    def partial(*refs):
        partial_body(rows, *refs)

    keep, send, places, digits = run(
        partial,
        (*halves(count // 2), S((2, count), I32), S((2 * chunks, LANES), F32)),
        projection,
        grad_out,
        token_ids.reshape(chunks, LANES),
        flops=2 * depth * count * hidden,
        limit=4,
    )
    keep, send = run(pair_body, halves(count // 4), keep, to_partner(send, 1), flops=keep.size, limit=4)
    looked = run(
        lookup,
        S((peers, width, count + count // 4), BF16),
        columns,
        places,
        keep,
        to_partner(send, 2),
        flops=2 * owners * width * rows * count,
        limit=8,
    )
    looked = exchange(looked, "hidden")

    made = run(
        products_body,
        S((members, piece + (chunks + 1) * SUBLANES, LANES), BF16),
        looked,
        grad_out,
        digits,
        flops=2 * depth * count * hidden,
        limit=8,
    )
    made = exchange(made, "vocab", groups)

    summed = run(
        group_sums,
        S((owners, piece + SUBLANES, LANES), BF16),
        made,
        flops=2 * members * count * owners * SUBLANES * LANES,
        limit=8,
    )
    summed = exchange(summed, "vocab")

    table_grad, projection_grad = run(
        last_sums, (S((width, rows), F32), S((depth, hidden), F32)), summed, flops=summed.size, limit=8
    )
    return table_grad.T, projection_grad


def solution(mesh):
    placed = (P("vocab"), P("vocab", None), P(None, "hidden"), P("vocab", "hidden"))
    return jax.shard_map(
        on_device,
        mesh=mesh,
        in_specs=placed,
        out_specs=(P("vocab", "hidden"), P(None, "hidden")),
        check_vma=False,
    )
```

```python
import jax
import jax.numpy as jnp
from jax import lax
from jax.experimental import pallas as pl
from jax.experimental.pallas import tpu as pltpu
from jax.sharding import PartitionSpec as P

F32, BF16, I32 = jnp.float32, jnp.bfloat16, jnp.int32
LANES, SUBLANES = 128, 8
AT_ONCE = 2
ALONG_Y = 8


def run(body, out, *args, flops, limit, space=pltpu.VMEM, scratch=(), specs=None):
    size = lambda a: a.size * a.dtype.itemsize
    vmem = pl.BlockSpec(memory_space=pltpu.VMEM)
    outs = jax.tree.leaves(out)
    if space != pltpu.VMEM:
        args = [pltpu.with_memory_space_constraint(a, space) for a in args]
    return pl.pallas_call(
        body,
        out_shape=out,
        in_specs=[pl.BlockSpec(memory_space=space)] * len(args),
        out_specs=specs or jax.tree.map(lambda _: vmem, out),
        scratch_shapes=scratch,
        compiler_params=pltpu.CompilerParams(vmem_limit_bytes=limit * 2**20),
        cost_estimate=pl.CostEstimate(
            flops=flops, bytes_accessed=sum(map(size, [*args, *outs])), transcendentals=0
        ),
    )(*args)


def exchange(blocks, axis, groups=None):
    return lax.all_to_all(blocks, axis, split_axis=0, concat_axis=0, tiled=True, axis_index_groups=groups)


def contract_last(a, b):
    return lax.dot_general(a, b, (((1,), (1,)), ((), ())), preferred_element_type=F32)


def one_hot_rows(which, rows):
    shape = (rows, which.shape[1])
    return (lax.broadcasted_iota(I32, shape, 0) == which).astype(F32).astype(BF16)


def owner_and_row(token, rows):
    owner = ((token >> 6) * 4370) >> 16
    return owner, token - owner * rows


def columns_body(table_there, ids_there, out, places, digits, table, ids, copied, arrivals):
    copies = [
        pltpu.make_async_copy(table_there, table, arrivals.at[0]),
        pltpu.make_async_copy(ids_there, ids, arrivals.at[1]),
    ]
    for copy in copies:
        copy.start()
    copies[0].wait()
    width = copied.shape[1] * 2
    first = lax.axis_index("hidden") * width
    shape = (width, table.shape[1])
    lane = lax.broadcasted_iota(I32, shape, 1)
    pick = (lane == lax.broadcasted_iota(I32, shape, 0) + first).astype(F32).astype(BF16)
    mine = contract_last(pick, table[...])
    half, whole = width // 2, table.shape[0] // LANES * LANES
    mine = jnp.concatenate(
        [mine[:half, :whole], mine[half:, :whole], mine[:half, whole:], mine[half:, whole:]], axis=1
    ).astype(BF16)
    at_once = copied.shape[0]
    for peer in range(at_once):
        copied[peer] = mine
    copies[1].wait()
    owner, row = owner_and_row(ids[...], table.shape[0])
    digits[...] = jnp.concatenate([owner * 8 + (row >> 7), row & 127], axis=0).astype(F32)
    for c in range(ids.shape[0]):
        at = slice(c * LANES, (c + 1) * LANES)
        places[0:1, at] = owner[c : c + 1]
        places[1:2, at] = row[c : c + 1]
    leaving = [
        pltpu.make_async_copy(copied, out.at[pl.ds(i * at_once, at_once)], arrivals.at[2 + i])
        for i in range(out.shape[0] // at_once)
    ]
    for copy in leaving:
        copy.start()
    for copy in leaving:
        copy.wait()


def split_lanes(value, upper, keep, send):
    half = value.shape[1] // 2
    low, high = value[:, :half], value[:, half:]
    keep[...] = jnp.where(upper, high, low)
    send[...] = jnp.where(upper, low, high).astype(BF16)


def partial_body(projection, grad_out, keep, send):
    upper = (lax.axis_index("hidden") & 1) == 1
    split_lanes(contract_last(projection[...], grad_out[...]), upper, keep, send)


def pair_body(kept, arrived, keep, send):
    upper = ((lax.axis_index("hidden") >> 1) & 1) == 1
    split_lanes(kept[...] + arrived[...].astype(F32), upper, keep, send)


def lookup_body(owners, table, places, kept, arrived, out):
    width = out.shape[1]
    count = places.shape[1]
    partial = kept[...] + arrived[...].astype(F32)
    owner, row = places[0:1, :], places[1:2, :]
    half = width // 2
    lines = table.shape[2]
    rows = lines // 2
    whole = rows // LANES * LANES
    held = table[...].reshape(owners * half, lines)
    both = jnp.concatenate([held[:, :whole], held[:, whole : 2 * whole]], axis=0)
    every = jnp.dot(both, one_hot_rows(row, whole), preferred_element_type=F32)
    rest = held[:, 2 * whole :]
    left = row - whole
    right = jnp.where(left >= 0, left + (rows - whole), -1)
    tails = [one_hot_rows(left, LANES // 2), one_hot_rows(right, LANES)]
    tails[0] = jnp.concatenate([tails[0], jnp.zeros_like(tails[0])], axis=0)
    first = every[: owners * half] + jnp.dot(rest, tails[0], preferred_element_type=F32)
    other = every[owners * half :] + jnp.dot(rest, tails[1], preferred_element_type=F32)
    pair = owner - (lax.broadcasted_iota(I32, (width, count), 0) >= half).astype(I32)
    sums = []
    for found in (first, other):
        total = jnp.zeros((width, count), F32)
        for v in range(0, owners, 2):
            total = jnp.where(pair == v, found[v * half : (v + 2) * half], total)
        sums.append(total[:half] + total[half:])
    total = jnp.concatenate(sums, axis=0)
    mine = total.astype(BF16)
    for peer in range(out.shape[0]):
        out[peer, :, :count] = mine
        out[peer, :, count:] = partial[peer * width : (peer + 1) * width].astype(BF16)


def rows_of_lanes(value):
    return [value[:, j : j + LANES] for j in range(0, value.shape[1], LANES)]


def products_body(arrived, grad_out, digits, out):
    peers = arrived.shape[0]
    count = grad_out.shape[0]
    embedded = jnp.concatenate([arrived[p, :, :count] for p in range(peers)], axis=0)
    product = jnp.dot(embedded, grad_out[...], preferred_element_type=F32)
    product = jnp.concatenate(rows_of_lanes(product), axis=0).astype(BF16)
    grads = []
    for core in range(2):
        for chip in range(2):
            senders = range(2 * chip + core, peers, 4)
            grads.append(sum(arrived[p, :, count:].astype(F32) for p in senders))
    small = [part.astype(BF16) for part in [*grads, digits[...]]]
    members = out.shape[0]
    piece = product.shape[0] // members
    for peer in range(members):
        out[peer, :piece] = product[peer * piece : (peer + 1) * piece]
        for c, part in enumerate(small):
            at = piece + c * SUBLANES
            out[peer, at : at + SUBLANES] = part


def group_sums_body(piece, arrived, out):
    members, owners = arrived.shape[0], out.shape[0]
    chunks = (arrived.shape[1] - piece) // SUBLANES - 1
    vocab = lax.axis_index("vocab")
    member = (vocab // ALONG_Y) * 2 + (vocab & 1)

    total = arrived[0, :piece].astype(F32)
    for peer in range(1, members):
        total = total + arrived[peer, :piece].astype(F32)
    total = total.astype(BF16)

    sums = jnp.zeros((owners * SUBLANES, LANES), F32)
    for peer in range(members):
        at = piece + chunks * SUBLANES
        digits = arrived[peer, at : at + SUBLANES].astype(F32).astype(I32)
        high, low = digits[:chunks], digits[chunks:]
        owner = jnp.where((high & 7) == member, high >> 3, -1)
        left, right = [], []
        for c in range(chunks):
            start = piece + c * SUBLANES
            part = arrived[peer, start : start + SUBLANES].astype(F32)
            owner_c = jnp.broadcast_to(owner[c : c + 1], part.shape)
            left.append(
                jnp.concatenate([jnp.where(owner_c == v, part, 0.0) for v in range(owners)], axis=0).astype(BF16)
            )
            right.append(one_hot_rows(low[c : c + 1], LANES))
        sums = sums + contract_last(jnp.concatenate(left, axis=1), jnp.concatenate(right, axis=1))
    sums = sums.astype(BF16)
    for v in range(owners):
        out[v, :piece] = total
        out[v, piece:] = sums[v * SUBLANES : (v + 1) * SUBLANES]


def last_sums_body(piece, arrived, table_grad, projection_grad):
    owners = arrived.shape[0]
    depth = projection_grad.shape[0]
    rows = table_grad.shape[1]
    members = depth * projection_grad.shape[1] // LANES // piece
    for member in range(members):
        first = (member >> 1) * ALONG_Y + (member & 1)
        total = arrived[first].astype(F32)
        for peer in range(first + 2, first + ALONG_Y, 2):
            total = total + arrived[peer].astype(F32)
        at, lane = member * piece % depth, member * piece // depth * LANES
        projection_grad[at : at + piece, lane : lane + LANES] = total[:piece]
        wide = min(LANES, rows - member * LANES)
        table_grad[:, member * LANES : member * LANES + wide] = total[piece:, :wide]


def on_device(token_ids, table, projection, grad_out):
    owners, peers = lax.axis_size("vocab"), lax.axis_size("hidden")
    along_x = owners // ALONG_Y
    members = 2 * along_x
    groups = [
        [x * ALONG_Y + y + bit for x in range(along_x) for bit in range(2)] for y in range(0, ALONG_Y, 2)
    ]
    rows, depth = table.shape
    width = depth // peers
    count = token_ids.shape[0]
    hidden = projection.shape[1]
    piece = depth * hidden // LANES // members
    chunks = count // LANES
    S = jax.ShapeDtypeStruct

    by_lane = token_ids.reshape(chunks, LANES)
    columns, places, digits = run(
        columns_body,
        (S((owners, width // 2, 2 * rows), BF16), S((2, count), I32), S((2 * chunks, LANES), F32)),
        table,
        by_lane,
        flops=2 * depth * rows * width,
        limit=4,
        space=pltpu.HBM,
        scratch=[
            pltpu.VMEM(table.shape, table.dtype),
            pltpu.VMEM(by_lane.shape, I32),
            pltpu.VMEM((AT_ONCE, width // 2, 2 * rows), BF16),
            pltpu.SemaphoreType.DMA((2 + owners // AT_ONCE,)),
        ],
        specs=tuple(pl.BlockSpec(memory_space=place) for place in (pltpu.HBM, pltpu.VMEM, pltpu.VMEM)),
    )
    columns = exchange(columns, "vocab")

    def lookup(*refs):
        lookup_body(owners, *refs)

    def group_sums(*refs):
        group_sums_body(piece, *refs)

    def last_sums(*refs):
        last_sums_body(piece, *refs)

    def to_partner(send, bit):
        return lax.ppermute(send, "hidden", [(i, i ^ bit) for i in range(peers)])

    def halves(columns):
        return (S((depth, columns), F32), S((depth, columns), BF16))

    keep, send = run(
        partial_body, halves(count // 2), projection, grad_out, flops=2 * depth * count * hidden, limit=4
    )
    keep, send = run(pair_body, halves(count // 4), keep, to_partner(send, 1), flops=keep.size, limit=4)
    looked = run(
        lookup,
        S((peers, width, count + count // 4), BF16),
        columns,
        places,
        keep,
        to_partner(send, 2),
        flops=2 * owners * width * rows * count,
        limit=8,
    )
    looked = exchange(looked, "hidden")

    made = run(
        products_body,
        S((members, piece + (chunks + 1) * SUBLANES, LANES), BF16),
        looked,
        grad_out,
        digits,
        flops=2 * depth * count * hidden,
        limit=8,
    )
    made = exchange(made, "vocab", groups)

    summed = run(
        group_sums,
        S((owners, piece + SUBLANES, LANES), BF16),
        made,
        flops=2 * members * count * owners * SUBLANES * LANES,
        limit=8,
    )
    summed = exchange(summed, "vocab")

    table_grad, projection_grad = run(
        last_sums, (S((width, rows), F32), S((depth, hidden), F32)), summed, flops=summed.size, limit=8
    )
    return table_grad.T, projection_grad


def solution(mesh):
    placed = (P("vocab"), P("vocab", None), P(None, "hidden"), P("vocab", "hidden"))
    return jax.shard_map(
        on_device,
        mesh=mesh,
        in_specs=placed,
        out_specs=(P("vocab", "hidden"), P(None, "hidden")),
        check_vma=False,
    )
```

```python
import jax
import jax.numpy as jnp
from jax import lax
from jax.experimental import pallas as pl
from jax.experimental.pallas import tpu as pltpu
from jax.sharding import PartitionSpec as P

F32, BF16, I32 = jnp.float32, jnp.bfloat16, jnp.int32
LANES, SUBLANES = 128, 8
AT_ONCE = 16
ALONG_Y = 8


def run(body, out, *args, flops, limit, space=pltpu.VMEM, scratch=(), specs=None):
    size = lambda a: a.size * a.dtype.itemsize
    vmem = pl.BlockSpec(memory_space=pltpu.VMEM)
    outs = jax.tree.leaves(out)
    if space != pltpu.VMEM:
        args = [pltpu.with_memory_space_constraint(a, space) for a in args]
    return pl.pallas_call(
        body,
        out_shape=out,
        in_specs=[pl.BlockSpec(memory_space=space)] * len(args),
        out_specs=specs or jax.tree.map(lambda _: vmem, out),
        scratch_shapes=scratch,
        compiler_params=pltpu.CompilerParams(vmem_limit_bytes=limit * 2**20),
        cost_estimate=pl.CostEstimate(
            flops=flops, bytes_accessed=sum(map(size, [*args, *outs])), transcendentals=0
        ),
    )(*args)


def exchange(blocks, axis, groups=None):
    return lax.all_to_all(blocks, axis, split_axis=0, concat_axis=0, tiled=True, axis_index_groups=groups)


def contract_last(a, b):
    return lax.dot_general(a, b, (((1,), (1,)), ((), ())), preferred_element_type=F32)


def one_hot_rows(which, rows):
    shape = (rows, which.shape[1])
    return (lax.broadcasted_iota(I32, shape, 0) == which).astype(F32).astype(BF16)


def owner_and_row(token, rows):
    owner = ((token >> 6) * 4370) >> 16
    return owner, token - owner * rows


def columns_body(table_there, ids_there, out, places, digits, table, ids, copied, arrivals):
    copies = [
        pltpu.make_async_copy(table_there, table, arrivals.at[0]),
        pltpu.make_async_copy(ids_there, ids, arrivals.at[1]),
    ]
    for copy in copies:
        copy.start()
    copies[0].wait()
    width = copied.shape[1] * 2
    first = lax.axis_index("hidden") * width
    shape = (width, table.shape[1])
    lane = lax.broadcasted_iota(I32, shape, 1)
    pick = (lane == lax.broadcasted_iota(I32, shape, 0) + first).astype(F32).astype(BF16)
    mine = contract_last(pick, table[...])
    half, whole = width // 2, table.shape[0] // LANES * LANES
    mine = jnp.concatenate(
        [mine[:half, :whole], mine[half:, :whole], mine[:half, whole:], mine[half:, whole:]], axis=1
    ).astype(BF16)
    at_once = copied.shape[0]
    for peer in range(at_once):
        copied[peer] = mine
    copies[1].wait()
    owner, row = owner_and_row(ids[...], table.shape[0])
    digits[...] = jnp.concatenate([owner * 8 + (row >> 7), row & 127], axis=0).astype(F32)
    for c in range(ids.shape[0]):
        at = slice(c * LANES, (c + 1) * LANES)
        places[0:1, at] = owner[c : c + 1]
        places[1:2, at] = row[c : c + 1]
    leaving = [
        pltpu.make_async_copy(copied, out.at[pl.ds(i * at_once, at_once)], arrivals.at[2 + i])
        for i in range(out.shape[0] // at_once)
    ]
    for copy in leaving:
        copy.start()
    for copy in leaving:
        copy.wait()


def split_lanes(value, upper, keep, send):
    half = value.shape[1] // 2
    low, high = value[:, :half], value[:, half:]
    keep[...] = jnp.where(upper, high, low)
    send[...] = jnp.where(upper, low, high).astype(BF16)


def partial_body(projection, grad_out, keep, send):
    upper = (lax.axis_index("hidden") & 1) == 1
    split_lanes(contract_last(projection[...], grad_out[...]), upper, keep, send)


def pair_body(kept, arrived, keep, send):
    upper = ((lax.axis_index("hidden") >> 1) & 1) == 1
    split_lanes(kept[...] + arrived[...].astype(F32), upper, keep, send)


def lookup_body(owners, table, places, kept, arrived, out):
    width = out.shape[1]
    count = places.shape[1]
    partial = kept[...] + arrived[...].astype(F32)
    owner, row = places[0:1, :], places[1:2, :]
    half = width // 2
    lines = table.shape[2]
    rows = lines // 2
    whole = rows // LANES * LANES
    held = table[...].reshape(owners * half, lines)
    both = jnp.concatenate([held[:, :whole], held[:, whole : 2 * whole]], axis=0)
    every = jnp.dot(both, one_hot_rows(row, whole), preferred_element_type=F32)
    rest = held[:, 2 * whole :]
    left = row - whole
    right = jnp.where(left >= 0, left + (rows - whole), -1)
    tails = [one_hot_rows(left, LANES // 2), one_hot_rows(right, LANES)]
    tails[0] = jnp.concatenate([tails[0], jnp.zeros_like(tails[0])], axis=0)
    first = every[: owners * half] + jnp.dot(rest, tails[0], preferred_element_type=F32)
    other = every[owners * half :] + jnp.dot(rest, tails[1], preferred_element_type=F32)
    pair = owner - (lax.broadcasted_iota(I32, (width, count), 0) >= half).astype(I32)
    sums = []
    for found in (first, other):
        total = jnp.zeros((width, count), F32)
        for v in range(0, owners, 2):
            total = jnp.where(pair == v, found[v * half : (v + 2) * half], total)
        sums.append(total[:half] + total[half:])
    total = jnp.concatenate(sums, axis=0)
    mine = total.astype(BF16)
    for peer in range(out.shape[0]):
        out[peer, :, :count] = mine
        out[peer, :, count:] = partial[peer * width : (peer + 1) * width].astype(BF16)


def rows_of_lanes(value):
    return [value[:, j : j + LANES] for j in range(0, value.shape[1], LANES)]


def products_body(arrived, grad_out, digits, out):
    peers = arrived.shape[0]
    count = grad_out.shape[0]
    embedded = jnp.concatenate([arrived[p, :, :count] for p in range(peers)], axis=0)
    product = jnp.dot(embedded, grad_out[...], preferred_element_type=F32)
    product = jnp.concatenate(rows_of_lanes(product), axis=0).astype(BF16)
    grads = []
    for core in range(2):
        for chip in range(2):
            senders = range(2 * chip + core, peers, 4)
            grads.append(sum(arrived[p, :, count:].astype(F32) for p in senders))
    small = [part.astype(BF16) for part in [*grads, digits[...]]]
    members = out.shape[0]
    piece = product.shape[0] // members
    for peer in range(members):
        out[peer, :piece] = product[peer * piece : (peer + 1) * piece]
        for c, part in enumerate(small):
            at = piece + c * SUBLANES
            out[peer, at : at + SUBLANES] = part


def group_sums_body(piece, arrived, out):
    members, owners = arrived.shape[0], out.shape[0]
    chunks = (arrived.shape[1] - piece) // SUBLANES - 1
    vocab = lax.axis_index("vocab")
    member = (vocab // ALONG_Y) * 2 + (vocab & 1)

    total = arrived[0, :piece].astype(F32)
    for peer in range(1, members):
        total = total + arrived[peer, :piece].astype(F32)
    total = total.astype(BF16)

    sums = jnp.zeros((owners * SUBLANES, LANES), F32)
    for peer in range(members):
        at = piece + chunks * SUBLANES
        digits = arrived[peer, at : at + SUBLANES].astype(F32).astype(I32)
        high, low = digits[:chunks], digits[chunks:]
        owner = jnp.where((high & 7) == member, high >> 3, -1)
        left, right = [], []
        for c in range(chunks):
            start = piece + c * SUBLANES
            part = arrived[peer, start : start + SUBLANES].astype(F32)
            owner_c = jnp.broadcast_to(owner[c : c + 1], part.shape)
            left.append(
                jnp.concatenate([jnp.where(owner_c == v, part, 0.0) for v in range(owners)], axis=0).astype(BF16)
            )
            right.append(one_hot_rows(low[c : c + 1], LANES))
        sums = sums + contract_last(jnp.concatenate(left, axis=1), jnp.concatenate(right, axis=1))
    sums = sums.astype(BF16)
    for v in range(owners):
        out[v, :piece] = total
        out[v, piece:] = sums[v * SUBLANES : (v + 1) * SUBLANES]


def last_sums_body(piece, arrived, table_grad, projection_grad):
    owners = arrived.shape[0]
    depth = projection_grad.shape[0]
    rows = table_grad.shape[1]
    members = depth * projection_grad.shape[1] // LANES // piece
    for member in range(members):
        first = (member >> 1) * ALONG_Y + (member & 1)
        total = arrived[first].astype(F32)
        for peer in range(first + 2, first + ALONG_Y, 2):
            total = total + arrived[peer].astype(F32)
        at, lane = member * piece % depth, member * piece // depth * LANES
        projection_grad[at : at + piece, lane : lane + LANES] = total[:piece]
        wide = min(LANES, rows - member * LANES)
        table_grad[:, member * LANES : member * LANES + wide] = total[piece:, :wide]


def on_device(token_ids, table, projection, grad_out):
    owners, peers = lax.axis_size("vocab"), lax.axis_size("hidden")
    along_x = owners // ALONG_Y
    members = 2 * along_x
    groups = [
        [x * ALONG_Y + y + bit for x in range(along_x) for bit in range(2)] for y in range(0, ALONG_Y, 2)
    ]
    rows, depth = table.shape
    width = depth // peers
    count = token_ids.shape[0]
    hidden = projection.shape[1]
    piece = depth * hidden // LANES // members
    chunks = count // LANES
    S = jax.ShapeDtypeStruct

    by_lane = token_ids.reshape(chunks, LANES)
    columns, places, digits = run(
        columns_body,
        (S((owners, width // 2, 2 * rows), BF16), S((2, count), I32), S((2 * chunks, LANES), F32)),
        table,
        by_lane,
        flops=2 * depth * rows * width,
        limit=4,
        space=pltpu.HBM,
        scratch=[
            pltpu.VMEM(table.shape, table.dtype),
            pltpu.VMEM(by_lane.shape, I32),
            pltpu.VMEM((AT_ONCE, width // 2, 2 * rows), BF16),
            pltpu.SemaphoreType.DMA((2 + owners // AT_ONCE,)),
        ],
        specs=tuple(pl.BlockSpec(memory_space=place) for place in (pltpu.HBM, pltpu.VMEM, pltpu.VMEM)),
    )
    columns = exchange(columns, "vocab")

    def lookup(*refs):
        lookup_body(owners, *refs)

    def group_sums(*refs):
        group_sums_body(piece, *refs)

    def last_sums(*refs):
        last_sums_body(piece, *refs)

    def to_partner(send, bit):
        return lax.ppermute(send, "hidden", [(i, i ^ bit) for i in range(peers)])

    def halves(columns):
        return (S((depth, columns), F32), S((depth, columns), BF16))

    keep, send = run(
        partial_body, halves(count // 2), projection, grad_out, flops=2 * depth * count * hidden, limit=4
    )
    keep, send = run(pair_body, halves(count // 4), keep, to_partner(send, 1), flops=keep.size, limit=4)
    looked = run(
        lookup,
        S((peers, width, count + count // 4), BF16),
        columns,
        places,
        keep,
        to_partner(send, 2),
        flops=2 * owners * width * rows * count,
        limit=8,
    )
    looked = exchange(looked, "hidden")

    made = run(
        products_body,
        S((members, piece + (chunks + 1) * SUBLANES, LANES), BF16),
        looked,
        grad_out,
        digits,
        flops=2 * depth * count * hidden,
        limit=8,
    )
    made = exchange(made, "vocab", groups)

    summed = run(
        group_sums,
        S((owners, piece + SUBLANES, LANES), BF16),
        made,
        flops=2 * members * count * owners * SUBLANES * LANES,
        limit=8,
    )
    summed = exchange(summed, "vocab")

    table_grad, projection_grad = run(
        last_sums, (S((width, rows), F32), S((depth, hidden), F32)), summed, flops=summed.size, limit=8
    )
    return table_grad.T, projection_grad


def solution(mesh):
    placed = (P("vocab"), P("vocab", None), P(None, "hidden"), P("vocab", "hidden"))
    return jax.shard_map(
        on_device,
        mesh=mesh,
        in_specs=placed,
        out_specs=(P("vocab", "hidden"), P(None, "hidden")),
        check_vma=False,
    )
```
